128 devices in a mesh: seq: 16 (over z, y_lo, core), kv: 8 (over y_hi, x).
Axes of the slice: x: 4, y: 4 (y_hi: 2, y_lo: 2; y = y_hi * 2 + y_lo), z: 4, core: 2. Of those that a mesh axis runs over, the one named last changes fastest.
Arguments:
- queries: bfloat16 [4096, 64, 128], P('seq', 'kv'), may hold values from -8 to 8
- keys: bfloat16 [4096, 8, 128], P('seq', 'kv'), may hold values from -8 to 8
- values: bfloat16 [4096, 8, 128], P('seq', 'kv'), may hold values from -6 to 6
- q_map: bfloat16 [64, 128, 128], P('kv'), may hold values from -0.5 to 0.5
- k_map: bfloat16 [8, 128, 128], P('kv'), may hold values from -0.5 to 0.5
- block_pairs: int32 [272, 2], replicated, may hold values from 0 to 31, as said below
Outputs:
- q_step: float32 [64, 128, 128], P('kv')
- k_step: float32 [8, 128, 128], P('kv')
- loss: float32 [], replicated
The draws below stay inside these ranges and needn't reach their ends.
Inputs may be any that keep to these rules, and one draw needn't show every extreme that they name: `block_pairs`: each row is a pair (query block, key block) of blocks of 128 tokens, the key block never after the query block; query block q appears with itself and with exactly q // 2 distinct earlier blocks; no pair appears twice.
All inputs are finite; a program needn't handle non-finite values.
Results may differ from the reference program's by a relative error of at most 0.015.
Values may be sent and summed in bfloat16 or wider, within the bound.
No kernel may reach another device: no remote copies, remote signals or barrier semaphores. Data moves between devices by JAX's collectives and lax.ppermute only.
A program may use at most 64 MiB of HBM per device.

```python
import math
import jax
import jax.numpy as jnp
from jax import lax

HD = 128
GROUP = 8
HALF = 128
KVH = 8
QH = 64
TOKENS = 4096
BLK = 128
NB = 32


def draw_queries(key, part):
    drawn = jnp.clip(jax.random.normal(jax.random.fold_in(key, 11), (TOKENS, QH, HD), jnp.float32), -6.0, 6.0)
    return drawn.astype(jnp.bfloat16)


def draw_keys(key, part):
    drawn = jnp.clip(jax.random.normal(jax.random.fold_in(key, 21), (TOKENS, KVH, HD), jnp.float32), -6.0, 6.0)
    return drawn.astype(jnp.bfloat16)


def draw_block_pairs(key, part):
    collected = []
    for query_index in range(NB):
        earlier = query_index // 2
        if earlier > 0:
            sub_key = jax.random.fold_in(key, 1000 + query_index)
            ranks = jax.random.randint(sub_key, (query_index,), 0, 1 << 20) * query_index + jnp.arange(query_index, dtype=jnp.int32)
            ranking = jnp.argsort(ranks, stable=True)
            chosen = ranking[:earlier].astype(jnp.int32)
            collected.append(jnp.stack([jnp.full((earlier,), query_index, jnp.int32), chosen], axis=1))
        collected.append(jnp.array([[query_index, query_index]], jnp.int32))
    return jnp.concatenate(collected, axis=0)


def shard_levels(own_key, dims, cuts, low, largest):
    gain, own = 1.0, jax.random.fold_in(own_key, 6)
    for axis_at, parts in cuts:
        draws = jnp.exp(jax.random.uniform(jax.random.fold_in(own, axis_at), (parts,), jnp.float32, low / len(cuts), largest / len(cuts)))
        gain = gain * jnp.repeat(draws, dims[axis_at] // parts).reshape([-1 if axis == axis_at else 1 for axis in range(len(dims))])
    return gain


def bell_draw(rng, extent, spread, reach, split=(), kind=jnp.bfloat16):
    values = jax.random.normal(rng, extent, jnp.float32) * spread
    if len(split) > 0:
        values = shard_levels(rng, extent, split, -0.22, 0.18) * values
    return jnp.clip(values, min=-reach, max=reach).astype(kind)


def setup_inputs(seed: int = 0) -> dict:
    arg_keys = jax.random.split(jax.random.key(seed), 7)
    queries = draw_queries(jax.random.fold_in(arg_keys[6], 71), 0)
    keys = draw_keys(jax.random.fold_in(arg_keys[6], 71), 0)
    values = bell_draw(arg_keys[2], (TOKENS, KVH, HD), 1.0, 6.0, ((0, 16), (1, 8)))
    q_map = bell_draw(arg_keys[3], (QH, HD, HALF), HD ** -0.5, 0.5, ((0, 8),))
    k_map = bell_draw(arg_keys[4], (KVH, HD, HALF), HD ** -0.5, 0.5, ((0, 8),))
    block_pairs = draw_block_pairs(jax.random.fold_in(arg_keys[6], 71), 0)
    return {"queries": queries, "keys": keys, "values": values, "q_map": q_map, "k_map": k_map, "block_pairs": block_pairs}


HIGHEST_PRECISION = lax.Precision.HIGHEST

def soft_pair(lifted):
    return jnp.concatenate([jax.nn.softmax(lifted, axis=-1), jax.nn.softmax(-lifted, axis=-1)], axis=-1)

def back_features(softened, upstream):
    half_width = softened.shape[-1] // 2
    leading, trailing = (softened[..., :half_width], softened[..., half_width:])
    up_lead, up_trail = (upstream[..., :half_width], upstream[..., half_width:])
    return leading * (up_lead - lax.optimization_barrier(jnp.sum(leading * up_lead, axis=-1, keepdims=True))) - trailing * (up_trail - lax.optimization_barrier(jnp.sum(trailing * up_trail, axis=-1, keepdims=True)))

def listed_mask(block_pairs):
    block_ids = jnp.arange(NB, dtype=jnp.int32)
    hit_query = (block_pairs[:, 0:1] == block_ids[None, :]).astype(jnp.float32)
    hit_key = (block_pairs[:, 1:2] == block_ids[None, :]).astype(jnp.float32)
    pair_table = jnp.dot(hit_query.T, hit_key, precision=HIGHEST_PRECISION) > 0.5
    positions = jnp.arange(TOKENS, dtype=jnp.int32)
    owning = (positions // BLK).astype(jnp.int32)
    expanded = jnp.take(jnp.take(pair_table, owning, axis=0), owning, axis=1)
    return expanded & (positions[:, None] >= positions[None, :])

def group_terms(key_rows, value_rows, key_weight, head_rows, head_weights, allowed):
    inv_root = 1.0 / math.sqrt(HD)
    soft_key = soft_pair(jnp.dot(key_rows, key_weight, preferred_element_type=jnp.float32))
    mapped_key = soft_key.astype(jnp.bfloat16)

    def one_head(items):
        query_rows, query_weight = items
        scores = jnp.dot(query_rows, key_rows.T, preferred_element_type=jnp.float32) * inv_root
        scores = jnp.where(allowed, scores, -1e+30)
        row_top = lax.optimization_barrier(jnp.max(scores, axis=-1, keepdims=True))
        weights = jnp.where(allowed, jnp.exp(scores - row_top), 0.0)
        teacher = jnp.dot(weights.astype(jnp.bfloat16), value_rows, preferred_element_type=jnp.float32) / lax.optimization_barrier(jnp.sum(weights, axis=-1, keepdims=True))
        soft_query = soft_pair(jnp.dot(query_rows, query_weight, preferred_element_type=jnp.float32))
        mapped_query = soft_query.astype(jnp.bfloat16)
        mixing = jnp.where(allowed, jnp.dot(mapped_query, mapped_key.T, preferred_element_type=jnp.float32), 0.0)
        student_norm = lax.optimization_barrier(jnp.sum(mixing, axis=-1, keepdims=True))
        student = jnp.dot(mixing.astype(jnp.bfloat16), value_rows, preferred_element_type=jnp.float32) / student_norm
        mismatch = student - teacher
        upstream = 2.0 * mismatch
        grad_num = (upstream / student_norm).astype(jnp.bfloat16)
        grad_norm = -lax.optimization_barrier(jnp.sum(upstream * student, axis=-1, keepdims=True)) / student_norm
        grad_mix = jnp.where(allowed, jnp.dot(grad_num, value_rows.T, preferred_element_type=jnp.float32) + grad_norm, 0.0).astype(jnp.bfloat16)
        grad_qf = jnp.dot(grad_mix, mapped_key, preferred_element_type=jnp.float32)
        grad_kf = jnp.dot(grad_mix.T, mapped_query, preferred_element_type=jnp.float32)
        grad_head = jnp.dot(query_rows.astype(jnp.float32).T, back_features(soft_query, grad_qf), precision=HIGHEST_PRECISION)
        return (grad_head, grad_kf, jnp.sum(mismatch * mismatch))
    head_grads, key_feature_grads, squares = lax.map(one_head, (head_rows, head_weights))
    summed_kf = lax.optimization_barrier(jnp.sum(key_feature_grads, axis=0))
    grad_key = jnp.dot(key_rows.astype(jnp.float32).T, back_features(soft_key, summed_kf), precision=HIGHEST_PRECISION)
    return (head_grads, grad_key, jnp.sum(squares))

def reference(queries, keys, values, q_map, k_map, block_pairs):
    allowed = listed_mask(block_pairs)
    head_rows = queries.reshape(TOKENS, KVH, GROUP, HD).transpose(1, 2, 0, 3)
    head_weights = q_map.reshape(KVH, GROUP, HD, HALF)
    key_rows = keys.transpose(1, 0, 2)
    value_rows = values.transpose(1, 0, 2)

    def one_group(items):
        return group_terms(items[0], items[1], items[2], items[3], items[4], allowed)
    head_grads, grad_keys, squares = lax.map(one_group, (key_rows, value_rows, k_map, head_rows, head_weights))
    grad_query = head_grads.reshape(QH, HD, HALF)
    squared = jnp.sum(grad_query * grad_query) + jnp.sum(grad_keys * grad_keys)
    scaling = jnp.sqrt(squared / ((QH + KVH) * HD * HALF) + 1e-06)
    loss = jnp.sum(squares) / (TOKENS * QH * HD)
    return (grad_query / scaling, grad_keys / scaling, loss)
```

```python
import math

import jax
import jax.numpy as jnp
from jax import lax
from jax.experimental import pallas as pl
from jax.experimental.pallas import tpu as pltpu
from jax.sharding import PartitionSpec as P


BLK = 128
HD = 128
HEADS = 8
SEQ = 16
KV = 8
SLOTS = 18
STEPS = SLOTS // 2
FLOOR = -1e30
LOG2E = 1.4426950408889634
ROWS = 72
PAYLOAD = 80
BF16 = jnp.bfloat16
F32 = jnp.float32

SAME_CORE = [[core + 2 * chip for chip in range(SEQ // 2)] for core in range(2)]
OTHER_CORE = [(i, i ^ 1) for i in range(SEQ)]
MIRROR = [(i, SEQ - 1 - i) for i in range(SEQ)]


def dot(a, b):
    return jnp.dot(a, b, preferred_element_type=F32)


def dot_nt(a, b):
    return lax.dot_general(a, b, (((1,), (1,)), ((), ())), preferred_element_type=F32)


def split_bf16(x):
    high = x.astype(BF16)
    return high, (x - high.astype(F32)).astype(BF16)


def halves(u, axis):
    top = jnp.max(u, axis=axis, keepdims=True)
    low = jnp.min(u, axis=axis, keepdims=True)
    up = jnp.exp(u - top)
    down = jnp.exp(low - u)
    up = up / jnp.sum(up, axis=axis, keepdims=True)
    down = down / jnp.sum(down, axis=axis, keepdims=True)
    return up, down


def list_blocks(mine, pairs, info):
    late = 2 * (SEQ - 1 - mine) + 1
    odd = lax.rem(mine, 2)
    for slot in range(SLOTS):
        info[slot] = 0
    info[0] = 2 * mine
    info[2] = late
    late_first = 4 + 2 * (mine // 2)

    def scan(row, counts):
        early_count, late_count = counts
        query = pairs[2 * row]
        key = pairs[2 * row + 1]
        earlier = query != key
        is_early = (query == 2 * mine) & earlier
        is_late = (query == late) & earlier

        @pl.when(is_early | is_late)
        def _():
            early_slot = jnp.where(early_count < odd, 1, 4 + early_count - odd)
            late_slot = jnp.where(late_count < 1 - odd, 3, late_first + late_count - (1 - odd))
            info[jnp.minimum(jnp.where(is_early, early_slot, late_slot), SLOTS - 1)] = key

        return (
            early_count + jnp.where(is_early, 1, 0),
            late_count + jnp.where(is_late, 1, 0),
        )

    lax.fori_loop(0, pairs.shape[0] // 2, scan, (jnp.int32(0), jnp.int32(0)))
    info[32] = jnp.where(odd == 1, 2 * BLK, -2 * BLK)
    info[33] = jnp.where(odd == 1, -2 * BLK, 2 * BLK)
    info[34] = 2 + mine // 2
    info[35] = odd


def features(q, q_map_t, q_t, mapped_t, mapped, soft_t):
    for head in range(HEADS):
        lanes = pl.ds(head * BLK, BLK)
        rows_t = q[head].T
        q_t[:, lanes] = rows_t
        up, down = halves(dot(q_map_t[head], rows_t), 0)
        soft = jnp.concatenate([up, down], axis=0)
        soft_t[:, lanes] = soft
        mapped_t[:, lanes] = soft.astype(BF16)
        mapped[lanes, :] = soft.T.astype(BF16)


def early_kernel(place, pairs, q, q_map_t, q_t, mapped_t, mapped, soft_t, info):
    list_blocks(place[0], pairs, info)
    features(q, q_map_t, q_t, mapped_t, mapped, soft_t)


def late_kernel(q, q_map_t, q_t, mapped_t, mapped, soft_t):
    features(q, q_map_t, q_t, mapped_t, mapped, soft_t)


def main_kernel(
    info, same, other, k_map,
    q_t0, mapped_t0, mapped0, soft_t0, q_t1, mapped_t1, mapped1, soft_t1,
    out,
    q_t, mapped_t, mapped, soft_t, kv, kv_sems, q_sems, v_t, k_t, soft_k, mk, mk_t,
    t_acc, s_acc, m_acc, l_acc, n_acc, gn, gnorm, gqf, gk_acc, flat, loss_acc,
    s_buf, p_buf, x_buf, kf_buf,
):
    parity = info[35]
    switch = info[34]

    def start_slot(slot):
        block = info[slot]
        chip = block // 4
        first = pl.multiple_of(lax.rem(block, 2) * BLK, BLK)
        near = lax.rem(block // 2, 2) == parity

        @pl.when(near)
        def _():
            pltpu.make_async_copy(
                same.at[chip, pl.ds(first, BLK)], kv.at[slot], kv_sems.at[slot]
            ).start()

        @pl.when(jnp.logical_not(near))
        def _():
            pltpu.make_async_copy(
                other.at[chip, pl.ds(first, BLK)], kv.at[slot], kv_sems.at[slot]
            ).start()

    def wait_slot(slot):
        pltpu.make_async_copy(same.at[0, pl.ds(0, BLK)], kv.at[slot], kv_sems.at[slot]).wait()

    loads = []
    for side, refs in enumerate(((q_t0, mapped_t0, mapped0, soft_t0), (q_t1, mapped_t1, mapped1, soft_t1))):
        for number, (ref, held) in enumerate(zip(refs, (q_t, mapped_t, mapped, soft_t))):
            loads.append(pltpu.make_async_copy(ref, held.at[side], q_sems.at[side, number]))
    for slot in range(4):
        start_slot(slot)
    loads[0].start()
    loads[1].start()
    loads[4].start()
    loads[5].start()
    for slot in range(4, SLOTS):
        start_slot(slot)
    for number in (2, 6, 3, 7):
        loads[number].start()

    def key_rows(step):
        return jnp.concatenate([kv[2 * step, :, :HD], kv[2 * step + 1, :, :HD]], axis=0)

    def value_rows(step):
        return jnp.concatenate([kv[2 * step, :, HD:], kv[2 * step + 1, :, HD:]], axis=0)

    def prepare(step):
        keys = key_rows(step)
        up, down = halves(dot(keys, k_map[...]), 1)
        soft = jnp.concatenate([up, down], axis=1)
        soft_k[step] = soft
        mk[step] = soft.astype(BF16)
        mk_t[step] = soft.T.astype(BF16)
        v_t[step] = value_rows(step).T
        k_t[step] = keys.T

    def allowed_of(side):
        key_minus_query = lax.broadcasted_iota(jnp.int32, (BLK, BLK), 0) - (
            lax.broadcasted_iota(jnp.int32, (BLK, BLK), 1)
        )
        tall = jnp.concatenate(
            [key_minus_query <= 0, key_minus_query <= info[32 + side]], axis=0
        )
        return jnp.concatenate([tall, tall], axis=1)

    shrink = LOG2E / math.sqrt(HD)
    wide = 2 * BLK
    chunks = HEADS // 2

    def forward(step, side, first):
        allowed = allowed_of(side) if first else None
        keys = key_rows(step)
        for c in range(chunks):
            lanes = pl.ds(c * wide, wide)
            scores = dot(keys, q_t[side, :, lanes])
            if first:
                scores = jnp.where(allowed, scores, FLOOR)
            s_buf[:, lanes] = scores
            new = jnp.max(scores, axis=0, keepdims=True)
            if first:
                m_acc[side, c] = new
            else:
                old = m_acc[side, c]
                new = jnp.maximum(old, new)
                m_acc[side, c] = new
                shift = jnp.exp2((old - new) * shrink)
                l_acc[side, c] = l_acc[side, c] * shift
                t_acc[side, c] = t_acc[side, c] * shift
        for c in range(chunks):
            lanes = pl.ds(c * wide, wide)
            mixing = dot(mk[step], mapped_t[side, :, lanes])
            if first:
                mixing = jnp.where(allowed, mixing, 0.0)
            total = jnp.sum(mixing, axis=0, keepdims=True)
            n_acc[side, c] = total if first else n_acc[side, c] + total
            x_buf[:, lanes] = mixing.astype(BF16)
        for c in range(chunks):
            lanes = pl.ds(c * wide, wide)
            weights = jnp.exp2((s_buf[:, lanes] - m_acc[side, c]) * shrink)
            total = jnp.sum(weights, axis=0, keepdims=True)
            l_acc[side, c] = total if first else l_acc[side, c] + total
            p_buf[:, lanes] = weights.astype(BF16)
        for c in range(chunks):
            lanes = pl.ds(c * wide, wide)
            product = dot(v_t[step], x_buf[:, lanes])
            s_acc[side, c] = product if first else s_acc[side, c] + product
        for c in range(chunks):
            lanes = pl.ds(c * wide, wide)
            product = dot(v_t[step], p_buf[:, lanes])
            t_acc[side, c] = product if first else t_acc[side, c] + product

    def wait_step(step):
        wait_slot(2 * step)
        wait_slot(2 * step + 1)

    def side_of(step):
        return jnp.where(step >= switch, 1, 0)

    wait_step(0)
    prepare(0)
    loads[0].wait()
    loads[1].wait()
    forward(0, 0, True)
    wait_step(1)
    prepare(1)
    loads[4].wait()
    loads[5].wait()
    wait_step(2)
    forward(1, 1, True)
    prepare(2)

    def forward_turn(step, carry):
        later = jnp.minimum(step + 1, STEPS - 1)

        @pl.when(step < STEPS - 1)
        def _():
            wait_step(later)

        forward(step, side_of(step), False)
        prepare(later)
        return carry

    lax.fori_loop(2, STEPS, forward_turn, 0)

    def settle(side, loss):
        for c in range(chunks):
            norm = 1.0 / n_acc[side, c]
            student = s_acc[side, c] * norm
            mismatch = student - t_acc[side, c] * (1.0 / l_acc[side, c])
            upstream = 2.0 * mismatch
            gn[side, c] = (upstream * norm).astype(BF16)
            gnorm[side, c] = -jnp.sum(upstream * student, axis=0, keepdims=True) * norm
            loss = loss + jnp.sum(mismatch * mismatch, axis=0, keepdims=True)
        return loss

    loss = lax.fori_loop(0, 2, settle, jnp.zeros((1, wide), F32))
    loss_acc[...] = jnp.broadcast_to(loss[:, :BLK] + loss[:, BLK:], loss_acc.shape)

    def key_back(step):
        grad_kf = kf_buf[...]
        soft = soft_k[step]
        lead, trail = soft[:, :HD], soft[:, HD:]
        g_lead, g_trail = grad_kf[:, :HD], grad_kf[:, HD:]
        back = lead * (g_lead - jnp.sum(lead * g_lead, axis=1, keepdims=True)) - trail * (
            g_trail - jnp.sum(trail * g_trail, axis=1, keepdims=True)
        )
        high, low = split_bf16(back)
        return dot(k_t[step], high) + dot(k_t[step], low)

    def backward(step, side, first):
        allowed = allowed_of(side) if first else None
        values = value_rows(step)
        for c in range(chunks):
            lanes = pl.ds(c * wide, wide)
            grad = dot(values, gn[side, c]) + gnorm[side, c]
            if first:
                grad = jnp.where(allowed, grad, 0.0)
            p_buf[:, lanes] = grad.astype(BF16)
        for c in range(chunks):
            lanes = pl.ds(c * wide, wide)
            product = dot(mk_t[step], p_buf[:, lanes])
            gqf[side, c] = product if first else gqf[side, c] + product
        kf_buf[...] = dot(p_buf[...], mapped[side])

    loads[2].wait()
    backward(0, 0, True)
    gk_acc[...] = key_back(0)
    loads[6].wait()
    backward(1, 1, True)

    def backward_turn(step, carry):
        gk_acc[...] = gk_acc[...] + key_back(step - 1)
        backward(step, side_of(step), False)
        return carry

    lax.fori_loop(2, STEPS, backward_turn, 0)
    loads[3].wait()
    loads[7].wait()
    flat[pl.ds(HEADS * HD, HD)] = gk_acc[...] + key_back(STEPS - 1)

    for head in range(HEADS):
        total = jnp.zeros((HD, HD), F32)
        lanes = pl.ds(head * BLK, BLK)
        column = (head % 2) * BLK
        for side in range(2):
            lead, trail = soft_t[side, :HD, lanes], soft_t[side, HD:, lanes]
            g_lead = gqf[side, head // 2, :HD, pl.ds(column, BLK)]
            g_trail = gqf[side, head // 2, HD:, pl.ds(column, BLK)]
            back = lead * (g_lead - jnp.sum(lead * g_lead, axis=0, keepdims=True)) - trail * (
                g_trail - jnp.sum(trail * g_trail, axis=0, keepdims=True)
            )
            high, low = split_bf16(back)
            rows_t = q_t[side, :, lanes]
            total = total + dot_nt(rows_t, high) + dot_nt(rows_t, low)
        flat[pl.ds(head * HD, HD)] = total
    high, low = split_bf16(loss_acc[...])
    tail = jnp.concatenate([high[:1], low[:1], jnp.zeros((6, BLK), BF16)], axis=0)
    for piece in range(SEQ):
        out[piece, pl.ds(0, ROWS)] = flat[pl.ds(piece * ROWS, ROWS)].astype(BF16)
        out[piece, pl.ds(ROWS, PAYLOAD - ROWS)] = tail


def fold_kernel(pieces, chunk, stats):
    total = jnp.sum(pieces[...].astype(F32), axis=0)
    grads = total[:ROWS]
    chunk[...] = grads.astype(BF16)
    squares = jnp.sum(grads * grads, axis=0, keepdims=True)
    loss = total[ROWS : ROWS + 1] + total[ROWS + 1 : ROWS + 2]
    rows = jnp.concatenate([squares, loss, jnp.zeros((6, BLK), F32)], axis=0)
    for peer in range(KV):
        stats[peer] = rows


def share_kernel(chunk, stats, payload, loss):
    total = jnp.sum(stats[...], axis=0)
    high, low = split_bf16(total)
    tail = jnp.concatenate([high[:1], low[:1], jnp.zeros((6, BLK), BF16)], axis=0)
    for peer in range(SEQ):
        payload[peer, pl.ds(0, ROWS)] = chunk[...]
        payload[peer, pl.ds(ROWS, PAYLOAD - ROWS)] = tail
    loss[...] = jnp.broadcast_to(
        jnp.sum(total[1:2], axis=1, keepdims=True) / (SEQ * 2 * BLK * KV * HEADS * HD), loss.shape
    )


def scale_kernel(pieces, q_out, k_out):
    tail = pieces[:, ROWS:, :].astype(F32)
    squared = jnp.sum(tail[:, 0, :] + tail[:, 1, :], axis=0, keepdims=True)
    squared = jnp.sum(squared, axis=1, keepdims=True)
    scale = jnp.sqrt(squared / ((HEADS + 1) * KV * HD * HD) + 1e-06)
    heads = HEADS * HD
    for piece in range(SEQ):
        rows = pieces[piece, pl.ds(0, ROWS)].astype(F32) / scale
        first = piece * ROWS
        keep = min(max(heads - first, 0), ROWS)
        if keep:
            q_out[pl.ds(first, keep)] = rows[:keep]
        if keep < ROWS:
            k_out[pl.ds(first + keep - heads, ROWS - keep)] = rows[keep:]


def vmem():
    return pl.BlockSpec(memory_space=pltpu.VMEM)


def smem():
    return pl.BlockSpec(memory_space=pltpu.SMEM)


def shape(dims, kind):
    return jax.ShapeDtypeStruct(dims, kind)


def any_space():
    return pl.BlockSpec(memory_space=pl.ANY)


def feature_shapes():
    wide = HEADS * BLK
    return (
        shape((HD, wide), BF16),
        shape((2 * HD, wide), BF16),
        shape((wide, 2 * HD), BF16),
        shape((2 * HD, wide), F32),
    )


def layer(queries, keys, values, q_map, k_map, block_pairs):
    place = lax.axis_index("seq").astype(jnp.int32).reshape(1)
    late = lax.ppermute(queries[BLK:], "seq", MIRROR)
    many = (SEQ // 2, 2 * BLK, HD)
    sent = jnp.concatenate(
        [jnp.broadcast_to(keys[:, 0, :], many), jnp.broadcast_to(values[:, 0, :], many)], axis=2
    )
    same = lax.all_to_all(sent, "seq", 0, 0, axis_index_groups=SAME_CORE, tiled=True)
    other = lax.ppermute(same, "seq", OTHER_CORE)

    cost = pl.CostEstimate(flops=5 * 10**9, bytes_accessed=10**7, transcendentals=10**6)
    q_map_t = jnp.transpose(q_map, (0, 2, 1))
    *early_parts, info = pl.pallas_call(
        early_kernel,
        out_shape=(*feature_shapes(), shape((128,), jnp.int32)),
        in_specs=[smem(), smem(), vmem(), vmem()],
        out_specs=(vmem(), vmem(), vmem(), vmem(), smem()),
        cost_estimate=cost,
        name="early_features",
    )(place, block_pairs.reshape(-1), jnp.transpose(queries[:BLK], (1, 0, 2)), q_map_t)
    late_parts = pl.pallas_call(
        late_kernel,
        out_shape=feature_shapes(),
        in_specs=[vmem(), vmem()],
        out_specs=(vmem(), vmem(), vmem(), vmem()),
        cost_estimate=cost,
        name="late_features",
    )(jnp.transpose(late, (1, 0, 2)), q_map_t)

    wide = HEADS * BLK
    pair = 2 * BLK
    chunks = HEADS // 2
    out = pl.pallas_call(
        main_kernel,
        out_shape=shape((SEQ, PAYLOAD, BLK), BF16),
        in_specs=[smem(), any_space(), any_space(), vmem()] + [any_space()] * 8,
        out_specs=vmem(),
        scratch_shapes=[
            pltpu.VMEM((2, HD, wide), BF16),
            pltpu.VMEM((2, 2 * HD, wide), BF16),
            pltpu.VMEM((2, wide, 2 * HD), BF16),
            pltpu.VMEM((2, 2 * HD, wide), F32),
            pltpu.VMEM((SLOTS, BLK, 2 * HD), BF16),
            pltpu.SemaphoreType.DMA((SLOTS,)),
            pltpu.SemaphoreType.DMA((2, 4)),
            pltpu.VMEM((STEPS, HD, pair), BF16),
            pltpu.VMEM((STEPS, HD, pair), BF16),
            pltpu.VMEM((STEPS, pair, 2 * HD), F32),
            pltpu.VMEM((STEPS, pair, 2 * HD), BF16),
            pltpu.VMEM((STEPS, 2 * HD, pair), BF16),
            pltpu.VMEM((2, chunks, HD, pair), F32),
            pltpu.VMEM((2, chunks, HD, pair), F32),
            pltpu.VMEM((2, chunks, 1, pair), F32),
            pltpu.VMEM((2, chunks, 1, pair), F32),
            pltpu.VMEM((2, chunks, 1, pair), F32),
            pltpu.VMEM((2, chunks, HD, pair), BF16),
            pltpu.VMEM((2, chunks, 1, pair), F32),
            pltpu.VMEM((2, chunks, 2 * HD, pair), F32),
            pltpu.VMEM((HD, HD), F32),
            pltpu.VMEM(((HEADS + 1) * HD, HD), F32),
            pltpu.VMEM((8, BLK), F32),
            pltpu.VMEM((pair, wide), F32),
            pltpu.VMEM((pair, wide), BF16),
            pltpu.VMEM((pair, wide), BF16),
            pltpu.VMEM((pair, 2 * HD), F32),
        ],
        compiler_params=pltpu.CompilerParams(vmem_limit_bytes=56 * 1024 * 1024),
        name="attend",
    )(info, same, other, k_map[0], *early_parts, *late_parts)

    pieces = lax.all_to_all(out, "seq", 0, 0, tiled=True)
    chunk, stats = pl.pallas_call(
        fold_kernel,
        out_shape=(shape((ROWS, BLK), BF16), shape((KV, 8, BLK), F32)),
        in_specs=[vmem()],
        out_specs=(vmem(), vmem()),
        name="fold",
    )(pieces)
    stats = lax.all_to_all(stats, "kv", 0, 0, tiled=True)
    payload, loss = pl.pallas_call(
        share_kernel,
        out_shape=(shape((SEQ, PAYLOAD, BLK), BF16), shape((8, BLK), F32)),
        in_specs=[vmem(), vmem()],
        out_specs=(vmem(), vmem()),
        name="share",
    )(chunk, stats)
    shared = lax.all_to_all(payload, "seq", 0, 0, tiled=True)
    grad_q, grad_k = pl.pallas_call(
        scale_kernel,
        out_shape=(shape((HEADS * HD, HD), F32), shape((HD, HD), F32)),
        in_specs=[vmem()],
        out_specs=(vmem(), vmem()),
        name="scale",
    )(shared)
    return grad_q.reshape(HEADS, HD, HD), grad_k.reshape(1, HD, HD), loss[0, 0]


def solution(mesh):
    placed = (
        P("seq", "kv", None),
        P("seq", "kv", None),
        P("seq", "kv", None),
        P("kv", None, None),
        P("kv", None, None),
        P(),
    )
    return jax.shard_map(
        layer,
        mesh=mesh,
        in_specs=placed,
        out_specs=(P("kv", None, None), P("kv", None, None), P()),
        check_vma=False,
    )
```

```python
import math

import jax
import jax.numpy as jnp
from jax import lax
from jax.experimental import pallas as pl
from jax.experimental.pallas import tpu as pltpu
from jax.sharding import PartitionSpec as P


BLK = 128
HD = 128
HEADS = 8
SEQ = 16
KV = 8
CHIPS = SEQ // 2
SLOTS = 18
STEPS = SLOTS // 2
UNROLL = 7
ATTEND_VMEM = 26 * 1024 * 1024
SMALL_VMEM = 4 * 1024 * 1024
FLOOR = -1e30
LOG2E = 1.4426950408889634
ROWS = 72
PAYLOAD = 80
BF16 = jnp.bfloat16
F32 = jnp.float32

SAME_CORE = [[core + 2 * chip for chip in range(SEQ // 2)] for core in range(2)]
OTHER_CORE = [(i, i ^ 1) for i in range(SEQ)]
MIRROR = [(i, SEQ - 1 - i) for i in range(SEQ)]


def dot(a, b):
    return jnp.dot(a, b, preferred_element_type=F32)


def dot_nt(a, b):
    return lax.dot_general(a, b, (((1,), (1,)), ((), ())), preferred_element_type=F32)


def split_bf16(x):
    high = x.astype(BF16)
    return high, (x - high.astype(F32)).astype(BF16)


def halves(u, axis):
    top = jnp.max(u, axis=axis, keepdims=True)
    low = jnp.min(u, axis=axis, keepdims=True)
    up = jnp.exp(u - top)
    down = jnp.exp(low - u)
    up = up / jnp.sum(up, axis=axis, keepdims=True)
    down = down / jnp.sum(down, axis=axis, keepdims=True)
    return up, down


def list_blocks(mine, pairs, info):
    late = 2 * (SEQ - 1 - mine) + 1
    odd = lax.rem(mine, 2)
    for slot in range(SLOTS):
        info[slot] = 0
    info[0] = 2 * mine
    info[2] = late
    late_first = 4 + 2 * (mine // 2)

    def scan(row, counts):
        early_count, late_count = counts
        query = pairs[2 * row]
        key = pairs[2 * row + 1]
        earlier = query != key
        is_early = (query == 2 * mine) & earlier
        is_late = (query == late) & earlier

        @pl.when(is_early | is_late)
        def _():
            early_slot = jnp.where(early_count < odd, 1, 4 + early_count - odd)
            late_slot = jnp.where(late_count < 1 - odd, 3, late_first + late_count - (1 - odd))
            info[jnp.minimum(jnp.where(is_early, early_slot, late_slot), SLOTS - 1)] = key

        return (
            early_count + jnp.where(is_early, 1, 0),
            late_count + jnp.where(is_late, 1, 0),
        )

    lax.fori_loop(0, pairs.shape[0] // 2, scan, (jnp.int32(0), jnp.int32(0)))
    info[32] = jnp.where(odd == 1, 2 * BLK, -2 * BLK)
    info[33] = jnp.where(odd == 1, -2 * BLK, 2 * BLK)
    info[34] = 2 + mine // 2
    info[35] = odd


def features(q, q_map_t, q_t, mapped_t, mapped, soft_t):
    for head in range(HEADS):
        lanes = pl.ds(head * BLK, BLK)
        rows_t = q[head].T
        q_t[:, lanes] = rows_t
        up, down = halves(dot(q_map_t[head], rows_t), 0)
        soft = jnp.concatenate([up, down], axis=0)
        soft_t[:, lanes] = soft
        rounded = soft.astype(BF16)
        mapped_t[:, lanes] = rounded
        mapped[lanes, :] = rounded.T


def list_kernel(place, pairs, info):
    list_blocks(place[0], pairs, info)


def main_kernel(
    info, same, other, k_map, early, late, q_map_t,
    near_out, far_out,
    q_t, mapped_t, mapped, soft_t, kv, v_t, k_t, soft_k, mk, mk_t,
    t_acc, s_acc, m_acc, l_acc, n_acc, gn, gnorm, gqf, gk_acc, flat, loss_acc,
    s_buf, x_raw, p_buf, x_buf, kf_buf, mk_next, v_next, shift_buf,
):
    parity = info[35]
    switch = info[34]

    def fetch(slot):
        block = info[slot]
        chip = block // 4
        rows = pl.ds(pl.multiple_of(lax.rem(block, 2) * BLK, BLK), BLK)
        near = lax.rem(block // 2, 2) == parity
        kv[slot] = jnp.where(near, same[chip, rows], other[chip, rows])

    def key_rows(step):
        return jnp.concatenate([kv[2 * step, :, :HD], kv[2 * step + 1, :, :HD]], axis=0)

    def value_rows(step):
        return jnp.concatenate([kv[2 * step, :, HD:], kv[2 * step + 1, :, HD:]], axis=0)

    def prepare(step):
        keys = key_rows(step)
        up, down = halves(dot(keys, k_map[...]), 1)
        soft_k[step, :, :HD] = up
        soft_k[step, :, HD:] = down
        up = up.astype(BF16)
        down = down.astype(BF16)
        mk_next[:, :HD] = up
        mk_next[:, HD:] = down
        mk_t[step, :HD] = up.T
        mk_t[step, HD:] = down.T
        v_next[...] = value_rows(step).T
        k_t[step] = keys.T

    def advance():
        mk[...] = mk_next[...]
        v_t[...] = v_next[...]

    def allowed_of(side):
        key_minus_query = lax.broadcasted_iota(jnp.int32, (BLK, BLK), 0) - (
            lax.broadcasted_iota(jnp.int32, (BLK, BLK), 1)
        )
        tall = jnp.concatenate(
            [key_minus_query <= 0, key_minus_query <= info[32 + side]], axis=0
        )
        return jnp.concatenate([tall, tall], axis=1)

    shrink = LOG2E / math.sqrt(HD)
    wide = 2 * BLK
    chunks = HEADS // 2

    tile = 64

    def over_sublanes(x, fold):
        return fold(x.reshape(x.shape[0] // 8, 8, x.shape[1]), axis=0)

    def forward(step, side, first, later):
        allowed = allowed_of(side) if first else None
        keys = key_rows(step)
        for c in range(chunks):
            lanes = pl.ds(c * wide, wide)
            s_buf[:, lanes] = dot(keys, q_t[side, :, lanes])
        for c in range(chunks):
            lanes = pl.ds(c * wide, wide)
            x_raw[:, lanes] = dot(mk[...], mapped_t[side, :, lanes])
        prepare(later)

        def masked(part, row, other):
            return jnp.where(allowed[row : row + tile], part, other) if first else part

        for c in range(chunks):
            lanes = pl.ds(c * wide, wide)
            best = jnp.full((8, wide), FLOOR, F32)
            for row in range(0, 2 * BLK, tile):
                part = masked(s_buf[pl.ds(row, tile), lanes], row, FLOOR)
                best = jnp.maximum(best, over_sublanes(part, jnp.max))
            new = jnp.max(best, axis=0, keepdims=True)
            if first:
                m_acc[side, c] = new
            else:
                old = m_acc[side, c]
                new = jnp.maximum(old, new)
                m_acc[side, c] = new
                shift = jnp.exp2((old - new) * shrink)
                shift_buf[c] = shift
            total = jnp.zeros((8, wide), F32)
            for row in range(0, 2 * BLK, tile):
                part = masked(s_buf[pl.ds(row, tile), lanes], row, FLOOR)
                weights = jnp.exp2((part - new) * shrink)
                total = total + over_sublanes(weights, jnp.sum)
                p_buf[pl.ds(row, tile), lanes] = weights.astype(BF16)
            l_acc[side, c] = total if first else l_acc[side, c] * shift + total
        for c in range(chunks):
            lanes = pl.ds(c * wide, wide)
            total = jnp.zeros((8, wide), F32)
            for row in range(0, 2 * BLK, tile):
                part = masked(x_raw[pl.ds(row, tile), lanes], row, 0.0)
                total = total + over_sublanes(part, jnp.sum)
                x_buf[pl.ds(row, tile), lanes] = part.astype(BF16)
            n_acc[side, c] = total if first else n_acc[side, c] + total
        for c in range(chunks):
            lanes = pl.ds(c * wide, wide)
            product = dot(v_t[...], x_buf[:, lanes])
            s_acc[side, c] = product if first else s_acc[side, c] + product
        for c in range(chunks):
            lanes = pl.ds(c * wide, wide)
            product = dot(v_t[...], p_buf[:, lanes])
            t_acc[side, c] = product if first else t_acc[side, c] * shift_buf[c] + product
        advance()

    def side_of(step):
        return jnp.where(step >= switch, 1, 0)

    for slot in range(SLOTS):
        fetch(slot)
    prepare(0)
    advance()
    for side, rows in enumerate((early, late)):
        features(rows, q_map_t, q_t.at[side], mapped_t.at[side], mapped.at[side], soft_t.at[side])
    forward(0, 0, True, 1)
    forward(1, 1, True, 2)

    def forward_turn(step, carry):
        forward(step, side_of(step), False, jnp.minimum(step + 1, STEPS - 1))
        return carry

    lax.fori_loop(2, STEPS, forward_turn, 0, unroll=UNROLL)

    def settle(side, loss):
        for c in range(chunks):
            norm = 1.0 / jnp.sum(n_acc[side, c], axis=0, keepdims=True)
            student = s_acc[side, c] * norm
            mass = 1.0 / jnp.sum(l_acc[side, c], axis=0, keepdims=True)
            mismatch = student - t_acc[side, c] * mass
            upstream = 2.0 * mismatch
            gn[side, c] = (upstream * norm).astype(BF16)
            gnorm[side, c] = -jnp.sum(upstream * student, axis=0, keepdims=True) * norm
            loss = loss + jnp.sum(mismatch * mismatch, axis=0, keepdims=True)
        return loss

    loss = lax.fori_loop(0, 2, settle, jnp.zeros((1, wide), F32))
    loss_acc[...] = jnp.broadcast_to(loss[:, :BLK] + loss[:, BLK:], loss_acc.shape)

    def key_back(step):
        grad_kf = kf_buf[...]
        soft = soft_k[step]
        lead, trail = soft[:, :HD], soft[:, HD:]
        g_lead, g_trail = grad_kf[:, :HD], grad_kf[:, HD:]
        back = lead * (g_lead - jnp.sum(lead * g_lead, axis=1, keepdims=True)) - trail * (
            g_trail - jnp.sum(trail * g_trail, axis=1, keepdims=True)
        )
        high, low = split_bf16(back)
        return dot(k_t[step], high) + dot(k_t[step], low)

    def backward(step, side, first):
        allowed = allowed_of(side) if first else None
        values = value_rows(step)
        for c in range(chunks):
            lanes = pl.ds(c * wide, wide)
            s_buf[:, lanes] = dot(values, gn[side, c])
        for c in range(chunks):
            lanes = pl.ds(c * wide, wide)
            for row in range(0, 2 * BLK, tile):
                part = s_buf[pl.ds(row, tile), lanes] + gnorm[side, c]
                if first:
                    part = jnp.where(allowed[row : row + tile], part, 0.0)
                p_buf[pl.ds(row, tile), lanes] = part.astype(BF16)
        for c in range(chunks):
            lanes = pl.ds(c * wide, wide)
            product = dot(mk_t[step], p_buf[:, lanes])
            gqf[side, c] = product if first else gqf[side, c] + product
        kf_buf[...] = dot(p_buf[...], mapped[side])

    backward(0, 0, True)
    gk_acc[...] = key_back(0)
    backward(1, 1, True)

    def backward_turn(step, carry):
        gk_acc[...] = gk_acc[...] + key_back(step - 1)
        backward(step, side_of(step), False)
        return carry

    lax.fori_loop(2, STEPS, backward_turn, 0, unroll=UNROLL)
    flat[pl.ds(HEADS * HD, HD)] = gk_acc[...] + key_back(STEPS - 1)

    for head in range(HEADS):
        total = jnp.zeros((HD, HD), F32)
        lanes = pl.ds(head * BLK, BLK)
        column = (head % 2) * BLK
        for side in range(2):
            lead, trail = soft_t[side, :HD, lanes], soft_t[side, HD:, lanes]
            g_lead = gqf[side, head // 2, :HD, pl.ds(column, BLK)]
            g_trail = gqf[side, head // 2, HD:, pl.ds(column, BLK)]
            back = lead * (g_lead - jnp.sum(lead * g_lead, axis=0, keepdims=True)) - trail * (
                g_trail - jnp.sum(trail * g_trail, axis=0, keepdims=True)
            )
            high, low = split_bf16(back)
            rows_t = q_t[side, :, lanes]
            total = total + dot_nt(rows_t, high) + dot_nt(rows_t, low)
        flat[pl.ds(head * HD, HD)] = total
    loss_row = loss_acc[:1]
    high, low = split_bf16(loss_row)
    rest = jnp.zeros((6, BLK), F32)
    near_tail = jnp.concatenate([loss_row, jnp.zeros((1, BLK), F32), rest], axis=0)
    far_tail = jnp.concatenate([high, low, rest.astype(BF16)], axis=0)
    for chip in range(CHIPS):
        near_row = pl.multiple_of((parity * CHIPS + chip) * ROWS, 8)
        far_row = pl.multiple_of(((1 - parity) * CHIPS + chip) * ROWS, 8)
        near_out[chip, pl.ds(0, ROWS)] = flat[pl.ds(near_row, ROWS)]
        near_out[chip, pl.ds(ROWS, PAYLOAD - ROWS)] = near_tail
        far_out[chip, pl.ds(0, ROWS)] = flat[pl.ds(far_row, ROWS)].astype(BF16)
        far_out[chip, pl.ds(ROWS, PAYLOAD - ROWS)] = far_tail


def fold_kernel(pieces, chunk, stats):
    total = jnp.sum(pieces[...].astype(F32), axis=0)
    grads = total[:ROWS]
    chunk[...] = grads.astype(BF16)
    squares = jnp.sum(grads * grads, axis=0, keepdims=True)
    loss = total[ROWS : ROWS + 1] + total[ROWS + 1 : ROWS + 2]
    rows = jnp.concatenate([squares, loss, jnp.zeros((6, BLK), F32)], axis=0)
    for peer in range(KV):
        stats[peer] = rows


def share_kernel(chunk, stats, payload, loss):
    total = jnp.sum(stats[...], axis=0)
    high, low = split_bf16(total)
    tail = jnp.concatenate([high[:1], low[:1], jnp.zeros((6, BLK), BF16)], axis=0)
    for peer in range(CHIPS):
        payload[peer, pl.ds(0, ROWS)] = chunk[...]
        payload[peer, pl.ds(ROWS, PAYLOAD - ROWS)] = tail
    loss[...] = jnp.broadcast_to(
        jnp.sum(total[1:2], axis=1, keepdims=True) / (SEQ * 2 * BLK * KV * HEADS * HD), loss.shape
    )


def scale_kernel(place, own, sibling, q_out, k_out):
    south = lax.rem(place[0], 2) == 0
    heads = HEADS * HD
    sides = (
        jnp.where(south, own[...], sibling[...]),
        jnp.where(south, sibling[...], own[...]),
    )
    squared = jnp.zeros((1, BLK), F32)
    for side in sides:
        tail = side[:, ROWS:, :].astype(F32)
        squared = squared + jnp.sum(tail[:, 0, :] + tail[:, 1, :], axis=0, keepdims=True)
    squared = jnp.sum(squared, axis=1, keepdims=True)
    inverse = 1.0 / jnp.sqrt(squared / ((HEADS + 1) * KV * HD * HD) + 1e-06)
    for piece in range(SEQ):
        rows = sides[piece // CHIPS][piece % CHIPS, :ROWS].astype(F32) * inverse
        first = piece * ROWS
        keep = min(max(heads - first, 0), ROWS)
        if keep:
            q_out[pl.ds(first, keep)] = rows[:keep]
        if keep < ROWS:
            k_out[pl.ds(first + keep - heads, ROWS - keep)] = rows[keep:]


def pack_kernel(keys, values, out, both, sems):
    takes = [
        pltpu.make_async_copy(keys, both.at[:, pl.ds(0, HD)], sems.at[0]),
        pltpu.make_async_copy(values, both.at[:, pl.ds(HD, HD)], sems.at[1]),
    ]
    for take in takes:
        take.start()
    for take in takes:
        take.wait()
    gives = [
        pltpu.make_async_copy(both, out.at[peer], sems.at[2 + peer]) for peer in range(CHIPS)
    ]
    for give in gives:
        give.start()
    for give in gives:
        give.wait()


def vmem():
    return pl.BlockSpec(memory_space=pltpu.VMEM)


def smem():
    return pl.BlockSpec(memory_space=pltpu.SMEM)


def shape(dims, kind):
    return jax.ShapeDtypeStruct(dims, kind)


def attend(info, same, other, k_map, early, late, q_map_t):
    wide = HEADS * BLK
    pair = 2 * BLK
    chunks = HEADS // 2
    return pl.pallas_call(
        main_kernel,
        out_shape=(shape((CHIPS, PAYLOAD, BLK), F32), shape((CHIPS, PAYLOAD, BLK), BF16)),
        in_specs=[smem()] + [vmem()] * 6,
        out_specs=(vmem(), vmem()),
        scratch_shapes=[
            pltpu.VMEM((2, HD, wide), BF16),
            pltpu.VMEM((2, 2 * HD, wide), BF16),
            pltpu.VMEM((2, wide, 2 * HD), BF16),
            pltpu.VMEM((2, 2 * HD, wide), F32),
            pltpu.VMEM((SLOTS, BLK, 2 * HD), BF16),
            pltpu.VMEM((HD, pair), BF16),
            pltpu.VMEM((STEPS, HD, pair), BF16),
            pltpu.VMEM((STEPS, pair, 2 * HD), F32),
            pltpu.VMEM((pair, 2 * HD), BF16),
            pltpu.VMEM((STEPS, 2 * HD, pair), BF16),
            pltpu.VMEM((2, chunks, HD, pair), F32),
            pltpu.VMEM((2, chunks, HD, pair), F32),
            pltpu.VMEM((2, chunks, 1, pair), F32),
            pltpu.VMEM((2, chunks, 8, pair), F32),
            pltpu.VMEM((2, chunks, 8, pair), F32),
            pltpu.VMEM((2, chunks, HD, pair), BF16),
            pltpu.VMEM((2, chunks, 1, pair), F32),
            pltpu.VMEM((2, chunks, 2 * HD, pair), F32),
            pltpu.VMEM((HD, HD), F32),
            pltpu.VMEM(((HEADS + 1) * HD, HD), F32),
            pltpu.VMEM((8, BLK), F32),
            pltpu.VMEM((pair, wide), F32),
            pltpu.VMEM((pair, wide), F32),
            pltpu.VMEM((pair, wide), BF16),
            pltpu.VMEM((pair, wide), BF16),
            pltpu.VMEM((pair, 2 * HD), F32),
            pltpu.VMEM((pair, 2 * HD), BF16),
            pltpu.VMEM((HD, pair), BF16),
            pltpu.VMEM((chunks, 1, pair), F32),
        ],
        compiler_params=pltpu.CompilerParams(vmem_limit_bytes=ATTEND_VMEM),
        name="attend",
    )(info, same, other, k_map, early, late, q_map_t)


def layer(queries, keys, values, q_map, k_map, block_pairs):
    place = lax.axis_index("seq").astype(jnp.int32).reshape(1)
    sent = pl.pallas_call(
        pack_kernel,
        out_shape=shape((CHIPS, 2 * BLK, 2 * HD), BF16),
        in_specs=[pl.BlockSpec(memory_space=pl.ANY)] * 2,
        out_specs=pl.BlockSpec(memory_space=pl.ANY),
        scratch_shapes=[
            pltpu.VMEM((2 * BLK, 2 * HD), BF16),
            pltpu.SemaphoreType.DMA((2 + CHIPS,)),
        ],
        compiler_params=pltpu.CompilerParams(vmem_limit_bytes=56 * 1024 * 1024),
        name="pack",
    )(keys[:, 0, :], values[:, 0, :])
    same = lax.all_to_all(sent, "seq", 0, 0, axis_index_groups=SAME_CORE, tiled=True)
    other = lax.ppermute(same, "seq", OTHER_CORE)

    early = jnp.transpose(queries[:BLK], (1, 0, 2))
    late = jnp.transpose(queries[BLK:], (1, 0, 2))
    late = lax.ppermute(late, "seq", MIRROR)
    q_map_t = jnp.transpose(q_map, (0, 2, 1))
    info = pl.pallas_call(
        list_kernel,
        out_shape=shape((128,), jnp.int32),
        in_specs=[smem(), smem()],
        out_specs=smem(),
        cost_estimate=pl.CostEstimate(flops=5 * 10**9, bytes_accessed=10**5, transcendentals=0),
        compiler_params=pltpu.CompilerParams(vmem_limit_bytes=SMALL_VMEM),
        name="list",
    )(place, block_pairs.reshape(-1))

    small = pltpu.CompilerParams(vmem_limit_bytes=SMALL_VMEM)
    near, far = attend(info, same, other, k_map[0], early, late, q_map_t)
    met = (near + lax.ppermute(far, "seq", OTHER_CORE).astype(F32)).astype(BF16)
    pieces = lax.all_to_all(met, "seq", 0, 0, axis_index_groups=SAME_CORE, tiled=True)
    chunk, stats = pl.pallas_call(
        fold_kernel,
        out_shape=(shape((ROWS, BLK), BF16), shape((KV, 8, BLK), F32)),
        in_specs=[vmem()],
        out_specs=(vmem(), vmem()),
        compiler_params=small,
        name="fold",
    )(pieces)
    stats = lax.all_to_all(stats, "kv", 0, 0, tiled=True)
    payload, loss = pl.pallas_call(
        share_kernel,
        out_shape=(shape((CHIPS, PAYLOAD, BLK), BF16), shape((8, BLK), F32)),
        in_specs=[vmem(), vmem()],
        out_specs=(vmem(), vmem()),
        compiler_params=small,
        name="share",
    )(chunk, stats)
    own = lax.all_to_all(payload, "seq", 0, 0, axis_index_groups=SAME_CORE, tiled=True)
    sibling = lax.ppermute(own, "seq", OTHER_CORE)
    grad_q, grad_k = pl.pallas_call(
        scale_kernel,
        out_shape=(shape((HEADS * HD, HD), F32), shape((HD, HD), F32)),
        in_specs=[smem(), vmem(), vmem()],
        out_specs=(vmem(), vmem()),
        compiler_params=small,
        name="scale",
    )(place, own, sibling)
    return grad_q.reshape(HEADS, HD, HD), grad_k.reshape(1, HD, HD), loss[0, 0]


def solution(mesh):
    placed = (
        P("seq", "kv", None),
        P("seq", "kv", None),
        P("seq", "kv", None),
        P("kv", None, None),
        P("kv", None, None),
        P(),
    )
    return jax.shard_map(
        layer,
        mesh=mesh,
        in_specs=placed,
        out_specs=(P("kv", None, None), P("kv", None, None), P()),
        check_vma=False,
    )
```

```python
import math

import jax
import jax.numpy as jnp
from jax import lax
from jax.experimental import pallas as pl
from jax.experimental.pallas import tpu as pltpu
from jax.sharding import PartitionSpec as P


BLK = 128
HD = 128
HEADS = 8
SEQ = 16
KV = 8
CHIPS = SEQ // 2
SLOTS = 18
STEPS = SLOTS // 2
ATTEND_VMEM = 34 * 1024 * 1024
SMALL_VMEM = 4 * 1024 * 1024
FLOOR = -1e30
LOG2E = 1.4426950408889634
ROWS = 72
PAYLOAD = 80
BF16 = jnp.bfloat16
F32 = jnp.float32

SAME_CORE = [[core + 2 * chip for chip in range(SEQ // 2)] for core in range(2)]
OTHER_CORE = [(i, i ^ 1) for i in range(SEQ)]
OTHER_ROW = [(i, i ^ 2) for i in range(SEQ)]
LAYER_SHIFTS = [[(i, (i + 4 * back) % SEQ) for i in range(SEQ)] for back in (1, 2, 3)]
MIRROR = [(i, SEQ - 1 - i) for i in range(SEQ)]


def dot(a, b):
    return jnp.dot(a, b, preferred_element_type=F32)


def dot_nt(a, b):
    return lax.dot_general(a, b, (((1,), (1,)), ((), ())), preferred_element_type=F32)


def split_bf16(x):
    high = x.astype(BF16)
    return high, (x - high.astype(F32)).astype(BF16)


def halves(u, axis):
    top = jnp.max(u, axis=axis, keepdims=True)
    low = jnp.min(u, axis=axis, keepdims=True)
    up = jnp.exp(u - top)
    down = jnp.exp(low - u)
    up = up / jnp.sum(up, axis=axis, keepdims=True)
    down = down / jnp.sum(down, axis=axis, keepdims=True)
    return up, down


def list_blocks(mine, pairs, info):
    late = 2 * (SEQ - 1 - mine) + 1
    odd = lax.rem(mine, 2)
    for slot in range(SLOTS):
        info[slot] = 0
    info[0] = 2 * mine
    info[2] = late
    late_first = 4 + 2 * (mine // 2)

    def scan(row, counts):
        early_count, late_count = counts
        query = pairs[2 * row]
        key = pairs[2 * row + 1]
        earlier = query != key
        is_early = (query == 2 * mine) & earlier
        is_late = (query == late) & earlier

        @pl.when(is_early | is_late)
        def _():
            early_slot = jnp.where(early_count < odd, 1, 4 + early_count - odd)
            late_slot = jnp.where(late_count < 1 - odd, 3, late_first + late_count - (1 - odd))
            info[jnp.minimum(jnp.where(is_early, early_slot, late_slot), SLOTS - 1)] = key

        return (
            early_count + jnp.where(is_early, 1, 0),
            late_count + jnp.where(is_late, 1, 0),
        )

    lax.fori_loop(0, pairs.shape[0] // 2, scan, (jnp.int32(0), jnp.int32(0)))
    info[32] = jnp.where(odd == 1, 2 * BLK, -2 * BLK)
    info[33] = jnp.where(odd == 1, -2 * BLK, 2 * BLK)
    info[34] = 2 + mine // 2
    info[35] = odd


def features(q, q_map_t, q_t, mapped_t, mapped, soft_t):
    for head in range(HEADS):
        lanes = pl.ds(head * BLK, BLK)
        rows_t = q[head].T
        q_t[:, lanes] = rows_t
        up, down = halves(dot(q_map_t[head], rows_t), 0)
        soft = jnp.concatenate([up, down], axis=0)
        soft_t[:, lanes] = soft
        rounded = soft.astype(BF16)
        mapped_t[:, lanes] = rounded
        mapped[lanes, :] = rounded.T


def list_kernel(place, pairs, info):
    list_blocks(place[0], pairs, info)


def main_kernel(
    info, same, other, k_map, early, late, q_map_t,
    near_out, far_out,
    q_t, mapped_t, mapped, soft_t, kv, v_t, k_t, soft_k, mk, mk_t,
    t_acc, s_acc, m_acc, l_acc, n_acc, gn, gnorm, gqf, gk_acc, flat, loss_acc,
    s_bufs, x_raws, p_bufs, x_bufs, kf_bufs, shift_bufs,
):
    parity = info[35]
    switch = info[34]

    def fetch(slot):
        block = info[slot]
        chip = block // 4
        rows = pl.ds(pl.multiple_of(lax.rem(block, 2) * BLK, BLK), BLK)
        near = lax.rem(block // 2, 2) == parity
        kv[slot] = jnp.where(near, same[chip, rows], other[chip, rows])

    def key_rows(step):
        return jnp.concatenate([kv[2 * step, :, :HD], kv[2 * step + 1, :, :HD]], axis=0)

    def value_rows(step):
        return jnp.concatenate([kv[2 * step, :, HD:], kv[2 * step + 1, :, HD:]], axis=0)

    def prepare(step):
        keys = key_rows(step)
        up, down = halves(dot(keys, k_map[...]), 1)
        soft_k[step, :, :HD] = up
        soft_k[step, :, HD:] = down
        up = up.astype(BF16)
        down = down.astype(BF16)
        mk[step, :, :HD] = up
        mk[step, :, HD:] = down
        mk_t[step, :HD] = up.T
        mk_t[step, HD:] = down.T
        v_t[step] = value_rows(step).T
        k_t[step] = keys.T

    def allowed_of(side):
        key_minus_query = lax.broadcasted_iota(jnp.int32, (BLK, BLK), 0) - (
            lax.broadcasted_iota(jnp.int32, (BLK, BLK), 1)
        )
        tall = jnp.concatenate(
            [key_minus_query <= 0, key_minus_query <= info[32 + side]], axis=0
        )
        return jnp.concatenate([tall, tall], axis=1)

    shrink = LOG2E / math.sqrt(HD)
    wide = 2 * BLK
    chunks = HEADS // 2

    tile = 64

    def over_sublanes(x, fold):
        return fold(x.reshape(x.shape[0] // 8, 8, x.shape[1]), axis=0)

    def side_of(step):
        if step < 2:
            return step
        return jnp.where(step >= switch, 1, 0)

    def forward_dots(step):
        side = side_of(step)
        s_buf, x_raw = s_bufs.at[step % 2], x_raws.at[step % 2]
        keys = key_rows(step)
        for c in range(chunks):
            lanes = pl.ds(c * wide, wide)
            s_buf[:, lanes] = dot(keys, q_t[side, :, lanes])
        for c in range(chunks):
            lanes = pl.ds(c * wide, wide)
            x_raw[:, lanes] = dot(mk[step], mapped_t[side, :, lanes])

    def forward(step):
        side, first = side_of(step), step < 2
        allowed = allowed_of(side) if first else None
        s_buf, x_raw = s_bufs.at[step % 2], x_raws.at[step % 2]
        p_buf, x_buf = p_bufs.at[step % 2], x_bufs.at[step % 2]
        shift_buf = shift_bufs.at[step % 2]

        def masked(part, row, other):
            return jnp.where(allowed[row : row + tile], part, other) if first else part

        for c in range(chunks):
            lanes = pl.ds(c * wide, wide)
            best = jnp.full((8, wide), FLOOR, F32)
            for row in range(0, 2 * BLK, tile):
                part = masked(s_buf[pl.ds(row, tile), lanes], row, FLOOR)
                best = jnp.maximum(best, over_sublanes(part, jnp.max))
            new = jnp.max(best, axis=0, keepdims=True)
            if first:
                m_acc[side, c] = new
            else:
                old = m_acc[side, c]
                new = jnp.maximum(old, new)
                m_acc[side, c] = new
                shift = jnp.exp2((old - new) * shrink)
                shift_buf[c] = shift
            total = jnp.zeros((8, wide), F32)
            for row in range(0, 2 * BLK, tile):
                part = masked(s_buf[pl.ds(row, tile), lanes], row, FLOOR)
                weights = jnp.exp2((part - new) * shrink)
                total = total + over_sublanes(weights, jnp.sum)
                p_buf[pl.ds(row, tile), lanes] = weights.astype(BF16)
            l_acc[side, c] = total if first else l_acc[side, c] * shift + total
        for c in range(chunks):
            lanes = pl.ds(c * wide, wide)
            total = jnp.zeros((8, wide), F32)
            for row in range(0, 2 * BLK, tile):
                part = masked(x_raw[pl.ds(row, tile), lanes], row, 0.0)
                total = total + over_sublanes(part, jnp.sum)
                x_buf[pl.ds(row, tile), lanes] = part.astype(BF16)
            n_acc[side, c] = total if first else n_acc[side, c] + total
        for c in range(chunks):
            lanes = pl.ds(c * wide, wide)
            product = dot(v_t[step], x_buf[:, lanes])
            s_acc[side, c] = product if first else s_acc[side, c] + product
        for c in range(chunks):
            lanes = pl.ds(c * wide, wide)
            product = dot(v_t[step], p_buf[:, lanes])
            t_acc[side, c] = product if first else t_acc[side, c] * shift_buf[c] + product

    for slot in range(SLOTS):
        fetch(slot)
    prepare(0)
    for side, rows in enumerate((early, late)):
        features(rows, q_map_t, q_t.at[side], mapped_t.at[side], mapped.at[side], soft_t.at[side])
    prepare(1)
    forward_dots(0)
    for step in range(STEPS):
        if step + 2 < STEPS:
            prepare(step + 2)
        if step + 1 < STEPS:
            forward_dots(step + 1)
        forward(step)

    def settle(side, loss):
        for c in range(chunks):
            norm = 1.0 / jnp.sum(n_acc[side, c], axis=0, keepdims=True)
            student = s_acc[side, c] * norm
            mass = 1.0 / jnp.sum(l_acc[side, c], axis=0, keepdims=True)
            mismatch = student - t_acc[side, c] * mass
            upstream = 2.0 * mismatch
            gn[side, c] = (upstream * norm).astype(BF16)
            gnorm[side, c] = -jnp.sum(upstream * student, axis=0, keepdims=True) * norm
            loss = loss + jnp.sum(mismatch * mismatch, axis=0, keepdims=True)
        return loss

    loss = lax.fori_loop(0, 2, settle, jnp.zeros((1, wide), F32))
    loss_acc[...] = jnp.broadcast_to(loss[:, :BLK] + loss[:, BLK:], loss_acc.shape)

    def key_back(step):
        grad_kf = kf_bufs[step % 2]
        soft = soft_k[step]
        lead, trail = soft[:, :HD], soft[:, HD:]
        g_lead, g_trail = grad_kf[:, :HD], grad_kf[:, HD:]
        back = lead * (g_lead - jnp.sum(lead * g_lead, axis=1, keepdims=True)) - trail * (
            g_trail - jnp.sum(trail * g_trail, axis=1, keepdims=True)
        )
        high, low = split_bf16(back)
        return dot(k_t[step], high) + dot(k_t[step], low)

    def backward_dots(step):
        side, first = side_of(step), step < 2
        allowed = allowed_of(side) if first else None
        s_buf, p_buf = s_bufs.at[step % 2], p_bufs.at[step % 2]
        values = value_rows(step)
        for c in range(chunks):
            lanes = pl.ds(c * wide, wide)
            s_buf[:, lanes] = dot(values, gn[side, c])
        for c in range(chunks):
            lanes = pl.ds(c * wide, wide)
            for row in range(0, 2 * BLK, tile):
                part = s_buf[pl.ds(row, tile), lanes] + gnorm[side, c]
                if first:
                    part = jnp.where(allowed[row : row + tile], part, 0.0)
                p_buf[pl.ds(row, tile), lanes] = part.astype(BF16)

    def backward(step):
        side, first = side_of(step), step < 2
        p_buf = p_bufs.at[step % 2]
        for c in range(chunks):
            lanes = pl.ds(c * wide, wide)
            product = dot(mk_t[step], p_buf[:, lanes])
            gqf[side, c] = product if first else gqf[side, c] + product
        kf_bufs[step % 2] = dot(p_buf[...], mapped[side])

    backward_dots(0)
    gk_acc[...] = jnp.zeros((HD, HD), F32)
    for step in range(STEPS):
        if step + 1 < STEPS:
            backward_dots(step + 1)
        backward(step)
        if step:
            gk_acc[...] = gk_acc[...] + key_back(step - 1)
    flat[pl.ds(HEADS * HD, HD)] = gk_acc[...] + key_back(STEPS - 1)

    for head in range(HEADS):
        total = jnp.zeros((HD, HD), F32)
        lanes = pl.ds(head * BLK, BLK)
        column = (head % 2) * BLK
        for side in range(2):
            lead, trail = soft_t[side, :HD, lanes], soft_t[side, HD:, lanes]
            g_lead = gqf[side, head // 2, :HD, pl.ds(column, BLK)]
            g_trail = gqf[side, head // 2, HD:, pl.ds(column, BLK)]
            back = lead * (g_lead - jnp.sum(lead * g_lead, axis=0, keepdims=True)) - trail * (
                g_trail - jnp.sum(trail * g_trail, axis=0, keepdims=True)
            )
            high, low = split_bf16(back)
            rows_t = q_t[side, :, lanes]
            total = total + dot_nt(rows_t, high) + dot_nt(rows_t, low)
        flat[pl.ds(head * HD, HD)] = total
    loss_row = loss_acc[:1]
    high, low = split_bf16(loss_row)
    rest = jnp.zeros((6, BLK), F32)
    near_tail = jnp.concatenate([loss_row, jnp.zeros((1, BLK), F32), rest], axis=0)
    far_tail = jnp.concatenate([high, low, rest.astype(BF16)], axis=0)
    for chip in range(CHIPS):
        near_row = pl.multiple_of((parity * CHIPS + chip) * ROWS, 8)
        far_row = pl.multiple_of(((1 - parity) * CHIPS + chip) * ROWS, 8)
        near_out[chip, pl.ds(0, ROWS)] = flat[pl.ds(near_row, ROWS)]
        near_out[chip, pl.ds(ROWS, PAYLOAD - ROWS)] = near_tail
        far_out[chip, pl.ds(0, ROWS)] = flat[pl.ds(far_row, ROWS)].astype(BF16)
        far_out[chip, pl.ds(ROWS, PAYLOAD - ROWS)] = far_tail


def fold_kernel(pieces, chunk, stats):
    total = jnp.sum(pieces[...].astype(F32), axis=0)
    grads = total[:ROWS]
    chunk[...] = grads.astype(BF16)
    squares = jnp.sum(grads * grads, axis=0, keepdims=True)
    loss = (total[ROWS : ROWS + 1] + total[ROWS + 1 : ROWS + 2]) * (1.0 / SEQ)
    half = BLK // 2
    row = jnp.concatenate(
        [squares[:, :half] + squares[:, half:], loss[:, :half] + loss[:, half:]], axis=1
    )
    stats[...] = jnp.broadcast_to(row[None], stats.shape)


def scale_kernel(place, stats, near, across, far, far_across, q_out, k_out, loss, flat):
    total = jnp.sum(stats[...], axis=0)
    left = lax.broadcasted_iota(jnp.int32, (1, BLK), 1) < BLK // 2
    squared = jnp.sum(jnp.where(left, total, 0.0), axis=1, keepdims=True)
    loss[...] = jnp.sum(jnp.where(left, 0.0, total), axis=1, keepdims=True) / (
        SEQ * 2 * BLK * KV * HEADS * HD
    )
    inverse = 1.0 / jnp.sqrt(squared / ((HEADS + 1) * KV * HD * HD) + 1e-06)
    mine = place[0]
    core = lax.rem(mine, 2)
    row = lax.rem(mine // 2, 2)
    layer_at = mine // 4
    for number, ref in enumerate((near, across, far, far_across)):
        owner_core = core if number < 2 else 1 - core
        owner_row = row if number % 2 == 0 else 1 - row
        for back in range(4):
            owner_layer = lax.rem(layer_at + 4 - back, 4)
            piece = owner_core * CHIPS + owner_layer * 2 + owner_row
            rows = ref[pl.ds(back * ROWS, ROWS)].astype(F32) * inverse
            flat[pl.ds(pl.multiple_of(piece * ROWS, 8), ROWS)] = rows
    q_out[...] = flat[: HEADS * HD]
    k_out[...] = flat[HEADS * HD :]


def pack_kernel(keys, values, out, both, sems):
    takes = [
        pltpu.make_async_copy(keys, both.at[:, pl.ds(0, HD)], sems.at[0]),
        pltpu.make_async_copy(values, both.at[:, pl.ds(HD, HD)], sems.at[1]),
    ]
    for take in takes:
        take.start()
    for take in takes:
        take.wait()
    gives = [
        pltpu.make_async_copy(both, out.at[peer], sems.at[2 + peer]) for peer in range(CHIPS)
    ]
    for give in gives:
        give.start()
    for give in gives:
        give.wait()


def vmem():
    return pl.BlockSpec(memory_space=pltpu.VMEM)


def smem():
    return pl.BlockSpec(memory_space=pltpu.SMEM)


def shape(dims, kind):
    return jax.ShapeDtypeStruct(dims, kind)


def attend(info, same, other, k_map, early, late, q_map_t):
    wide = HEADS * BLK
    pair = 2 * BLK
    chunks = HEADS // 2
    return pl.pallas_call(
        main_kernel,
        out_shape=(shape((CHIPS, PAYLOAD, BLK), F32), shape((CHIPS, PAYLOAD, BLK), BF16)),
        in_specs=[smem()] + [vmem()] * 6,
        out_specs=(vmem(), vmem()),
        scratch_shapes=[
            pltpu.VMEM((2, HD, wide), BF16),
            pltpu.VMEM((2, 2 * HD, wide), BF16),
            pltpu.VMEM((2, wide, 2 * HD), BF16),
            pltpu.VMEM((2, 2 * HD, wide), F32),
            pltpu.VMEM((SLOTS, BLK, 2 * HD), BF16),
            pltpu.VMEM((STEPS, HD, pair), BF16),
            pltpu.VMEM((STEPS, HD, pair), BF16),
            pltpu.VMEM((STEPS, pair, 2 * HD), F32),
            pltpu.VMEM((STEPS, pair, 2 * HD), BF16),
            pltpu.VMEM((STEPS, 2 * HD, pair), BF16),
            pltpu.VMEM((2, chunks, HD, pair), F32),
            pltpu.VMEM((2, chunks, HD, pair), F32),
            pltpu.VMEM((2, chunks, 1, pair), F32),
            pltpu.VMEM((2, chunks, 8, pair), F32),
            pltpu.VMEM((2, chunks, 8, pair), F32),
            pltpu.VMEM((2, chunks, HD, pair), BF16),
            pltpu.VMEM((2, chunks, 1, pair), F32),
            pltpu.VMEM((2, chunks, 2 * HD, pair), F32),
            pltpu.VMEM((HD, HD), F32),
            pltpu.VMEM(((HEADS + 1) * HD, HD), F32),
            pltpu.VMEM((8, BLK), F32),
            pltpu.VMEM((2, pair, wide), F32),
            pltpu.VMEM((2, pair, wide), F32),
            pltpu.VMEM((2, pair, wide), BF16),
            pltpu.VMEM((2, pair, wide), BF16),
            pltpu.VMEM((2, pair, 2 * HD), F32),
            pltpu.VMEM((2, chunks, 1, pair), F32),
        ],
        compiler_params=pltpu.CompilerParams(vmem_limit_bytes=ATTEND_VMEM),
        name="attend",
    )(info, same, other, k_map, early, late, q_map_t)


def layer(queries, keys, values, q_map, k_map, block_pairs):
    place = lax.axis_index("seq").astype(jnp.int32).reshape(1)
    sent = pl.pallas_call(
        pack_kernel,
        out_shape=shape((CHIPS, 2 * BLK, 2 * HD), BF16),
        in_specs=[pl.BlockSpec(memory_space=pl.ANY)] * 2,
        out_specs=pl.BlockSpec(memory_space=pl.ANY),
        scratch_shapes=[
            pltpu.VMEM((2 * BLK, 2 * HD), BF16),
            pltpu.SemaphoreType.DMA((2 + CHIPS,)),
        ],
        compiler_params=pltpu.CompilerParams(vmem_limit_bytes=56 * 1024 * 1024),
        name="pack",
    )(keys[:, 0, :], values[:, 0, :])
    same = lax.all_to_all(sent, "seq", 0, 0, axis_index_groups=SAME_CORE, tiled=True)
    other = lax.ppermute(same, "seq", OTHER_CORE)

    early = jnp.transpose(queries[:BLK], (1, 0, 2))
    late = jnp.transpose(queries[BLK:], (1, 0, 2))
    late = lax.ppermute(late, "seq", MIRROR)
    q_map_t = jnp.transpose(q_map, (0, 2, 1))
    info = pl.pallas_call(
        list_kernel,
        out_shape=shape((128,), jnp.int32),
        in_specs=[smem(), smem()],
        out_specs=smem(),
        cost_estimate=pl.CostEstimate(flops=5 * 10**9, bytes_accessed=10**5, transcendentals=0),
        compiler_params=pltpu.CompilerParams(vmem_limit_bytes=SMALL_VMEM),
        name="list",
    )(place, block_pairs.reshape(-1))

    small = pltpu.CompilerParams(vmem_limit_bytes=SMALL_VMEM)
    near, far = attend(info, same, other, k_map[0], early, late, q_map_t)
    met = (near + lax.ppermute(far, "seq", OTHER_CORE).astype(F32)).astype(BF16)
    pieces = lax.all_to_all(met, "seq", 0, 0, axis_index_groups=SAME_CORE, tiled=True)
    everyone = SEQ * KV
    chunk, stats = pl.pallas_call(
        fold_kernel,
        out_shape=(shape((ROWS, BLK), BF16), shape((everyone, 1, BLK), F32)),
        in_specs=[vmem()],
        out_specs=(vmem(), vmem()),
        compiler_params=small,
        name="fold",
    )(pieces)
    stats = lax.all_to_all(stats, ("seq", "kv"), 0, 0, tiled=True)
    column = [chunk] + [lax.ppermute(chunk, "seq", route) for route in LAYER_SHIFTS]
    near = jnp.concatenate(column, axis=0)
    across = lax.ppermute(near, "seq", OTHER_ROW)
    far = lax.ppermute(near, "seq", OTHER_CORE)
    far_across = lax.ppermute(across, "seq", OTHER_CORE)
    grad_q, grad_k, loss = pl.pallas_call(
        scale_kernel,
        out_shape=(shape((HEADS * HD, HD), F32), shape((HD, HD), F32), shape((1, 1), F32)),
        in_specs=[smem()] + [vmem()] * 5,
        out_specs=(vmem(), vmem(), vmem()),
        scratch_shapes=[pltpu.VMEM(((HEADS + 1) * HD, HD), F32)],
        compiler_params=small,
        name="scale",
    )(place, stats, near, across, far, far_across)
    return grad_q.reshape(HEADS, HD, HD), grad_k.reshape(1, HD, HD), loss.reshape(())


def solution(mesh):
    placed = (
        P("seq", "kv", None),
        P("seq", "kv", None),
        P("seq", "kv", None),
        P("kv", None, None),
        P("kv", None, None),
        P(),
    )
    return jax.shard_map(
        layer,
        mesh=mesh,
        in_specs=placed,
        out_specs=(P("kv", None, None), P("kv", None, None), P()),
        check_vma=False,
    )
```

```python
import math

import jax
import jax.numpy as jnp
from jax import lax
from jax.experimental import pallas as pl
from jax.experimental.pallas import tpu as pltpu
from jax.sharding import PartitionSpec as P


BLK = 128
HD = 128
HEADS = 8
SEQ = 16
KV = 8
CHIPS = SEQ // 2
SLOTS = 18
STEPS = SLOTS // 2
ATTEND_VMEM = 34 * 1024 * 1024
SMALL_VMEM = 4 * 1024 * 1024
FLOOR = -1e30
LOG2E = 1.4426950408889634
ROWS = 72
PAYLOAD = 80
BF16 = jnp.bfloat16
F32 = jnp.float32

SAME_CORE = [[core + 2 * chip for chip in range(SEQ // 2)] for core in range(2)]
OTHER_CORE = [(i, i ^ 1) for i in range(SEQ)]
OTHER_ROW = [(i, i ^ 2) for i in range(SEQ)]
LAYER_SHIFTS = [[(i, (i + 4 * back) % SEQ) for i in range(SEQ)] for back in (1, 2, 3)]
MIRROR = [(i, SEQ - 1 - i) for i in range(SEQ)]


def dot(a, b):
    return jnp.dot(a, b, preferred_element_type=F32)


def dot_nt(a, b):
    return lax.dot_general(a, b, (((1,), (1,)), ((), ())), preferred_element_type=F32)


def split_bf16(x):
    high = x.astype(BF16)
    return high, (x - high.astype(F32)).astype(BF16)


def halves(u, axis):
    top = jnp.max(u, axis=axis, keepdims=True)
    low = jnp.min(u, axis=axis, keepdims=True)
    up = jnp.exp(u - top)
    down = jnp.exp(low - u)
    up = up / jnp.sum(up, axis=axis, keepdims=True)
    down = down / jnp.sum(down, axis=axis, keepdims=True)
    return up, down


def list_blocks(mine, pairs, info):
    late = 2 * (SEQ - 1 - mine) + 1
    odd = lax.rem(mine, 2)
    for slot in range(SLOTS):
        info[slot] = 0
    info[0] = 2 * mine
    info[2] = late
    late_first = 4 + 2 * (mine // 2)

    def scan(row, counts):
        early_count, late_count = counts
        query = pairs[2 * row]
        key = pairs[2 * row + 1]
        earlier = query != key
        is_early = (query == 2 * mine) & earlier
        is_late = (query == late) & earlier

        @pl.when(is_early | is_late)
        def _():
            early_slot = jnp.where(early_count < odd, 1, 4 + early_count - odd)
            late_slot = jnp.where(late_count < 1 - odd, 3, late_first + late_count - (1 - odd))
            info[jnp.minimum(jnp.where(is_early, early_slot, late_slot), SLOTS - 1)] = key

        return (
            early_count + jnp.where(is_early, 1, 0),
            late_count + jnp.where(is_late, 1, 0),
        )

    lax.fori_loop(0, pairs.shape[0] // 2, scan, (jnp.int32(0), jnp.int32(0)))
    info[32] = jnp.where(odd == 1, 2 * BLK, -2 * BLK)
    info[33] = jnp.where(odd == 1, -2 * BLK, 2 * BLK)
    info[34] = 2 + mine // 2
    info[35] = odd


def features(q, q_map_t, q_t, mapped_t, mapped, soft_t):
    for head in range(HEADS):
        lanes = pl.ds(head * BLK, BLK)
        rows_t = q[head].T
        q_t[:, lanes] = rows_t
        up, down = halves(dot(q_map_t[head], rows_t), 0)
        soft = jnp.concatenate([up, down], axis=0)
        soft_t[:, lanes] = soft
        rounded = soft.astype(BF16)
        mapped_t[:, lanes] = rounded
        mapped[lanes, :] = rounded.T


def list_kernel(place, pairs, info):
    list_blocks(place[0], pairs, info)


def main_kernel(
    info, same, other, k_map, early, late, q_map_t,
    near_out, far_out,
    q_t, mapped_t, mapped, soft_t, kv, v_t, k_t, soft_k, mk, mk_t,
    t_acc, s_acc, m_acc, l_acc, n_acc, gn, gnorm, gqf, gk_acc, flat, loss_acc,
    s_bufs, x_raws, p_bufs, x_bufs, kf_bufs, shift_bufs,
):
    parity = info[35]
    switch = info[34]

    def fetch(slot):
        block = info[slot]
        chip = block // 4
        rows = pl.ds(pl.multiple_of(lax.rem(block, 2) * BLK, BLK), BLK)
        near = lax.rem(block // 2, 2) == parity
        kv[slot] = jnp.where(near, same[chip, rows], other[chip, rows])

    def key_rows(step):
        return jnp.concatenate([kv[2 * step, :, :HD], kv[2 * step + 1, :, :HD]], axis=0)

    def value_rows(step):
        return jnp.concatenate([kv[2 * step, :, HD:], kv[2 * step + 1, :, HD:]], axis=0)

    def prepare(step):
        keys = key_rows(step)
        up, down = halves(dot(keys, k_map[...]), 1)
        soft_k[step, :, :HD] = up
        soft_k[step, :, HD:] = down
        up = up.astype(BF16)
        down = down.astype(BF16)
        mk[step, :, :HD] = up
        mk[step, :, HD:] = down
        mk_t[step, :HD] = up.T
        mk_t[step, HD:] = down.T
        v_t[step] = value_rows(step).T
        k_t[step] = keys.T

    def allowed_of(side):
        key_minus_query = lax.broadcasted_iota(jnp.int32, (BLK, BLK), 0) - (
            lax.broadcasted_iota(jnp.int32, (BLK, BLK), 1)
        )
        tall = jnp.concatenate(
            [key_minus_query <= 0, key_minus_query <= info[32 + side]], axis=0
        )
        return jnp.concatenate([tall, tall], axis=1)

    shrink = LOG2E / math.sqrt(HD)
    wide = 2 * BLK
    chunks = HEADS // 2

    tile = 64

    def over_sublanes(x, fold):
        return fold(x.reshape(x.shape[0] // 8, 8, x.shape[1]), axis=0)

    def side_of(step):
        if step < 2:
            return step
        return jnp.where(step >= switch, 1, 0)

    def forward_dots(step):
        side = side_of(step)
        s_buf, x_raw = s_bufs.at[step % 2], x_raws.at[step % 2]
        keys = key_rows(step)
        for c in range(chunks):
            lanes = pl.ds(c * wide, wide)
            s_buf[:, lanes] = dot(keys, q_t[side, :, lanes])
        for c in range(chunks):
            lanes = pl.ds(c * wide, wide)
            x_raw[:, lanes] = dot(mk[step], mapped_t[side, :, lanes])

    def forward(step):
        side, first = side_of(step), step < 2
        allowed = allowed_of(side) if first else None
        s_buf, x_raw = s_bufs.at[step % 2], x_raws.at[step % 2]
        p_buf, x_buf = p_bufs.at[step % 2], x_bufs.at[step % 2]
        shift_buf = shift_bufs.at[step % 2]

        def masked(part, row, other):
            return jnp.where(allowed[row : row + tile], part, other) if first else part

        for c in range(chunks):
            lanes = pl.ds(c * wide, wide)
            best = jnp.full((8, wide), FLOOR, F32)
            for row in range(0, 2 * BLK, tile):
                part = masked(s_buf[pl.ds(row, tile), lanes], row, FLOOR)
                best = jnp.maximum(best, over_sublanes(part, jnp.max))
            new = jnp.max(best, axis=0, keepdims=True)
            if first:
                m_acc[side, c] = new
            else:
                old = m_acc[side, c]
                new = jnp.maximum(old, new)
                m_acc[side, c] = new
                shift = jnp.exp2((old - new) * shrink)
                shift_buf[c] = shift
            total = jnp.zeros((8, wide), F32)
            for row in range(0, 2 * BLK, tile):
                part = masked(s_buf[pl.ds(row, tile), lanes], row, FLOOR)
                weights = jnp.exp2((part - new) * shrink)
                total = total + over_sublanes(weights, jnp.sum)
                p_buf[pl.ds(row, tile), lanes] = weights.astype(BF16)
            l_acc[side, c] = total if first else l_acc[side, c] * shift + total
        for c in range(chunks):
            lanes = pl.ds(c * wide, wide)
            total = jnp.zeros((8, wide), F32)
            for row in range(0, 2 * BLK, tile):
                part = masked(x_raw[pl.ds(row, tile), lanes], row, 0.0)
                total = total + over_sublanes(part, jnp.sum)
                x_buf[pl.ds(row, tile), lanes] = part.astype(BF16)
            n_acc[side, c] = total if first else n_acc[side, c] + total
        for c in range(chunks):
            lanes = pl.ds(c * wide, wide)
            product = dot(v_t[step], x_buf[:, lanes])
            s_acc[side, c] = product if first else s_acc[side, c] + product
        for c in range(chunks):
            lanes = pl.ds(c * wide, wide)
            product = dot(v_t[step], p_buf[:, lanes])
            t_acc[side, c] = product if first else t_acc[side, c] * shift_buf[c] + product

    for slot in range(SLOTS):
        fetch(slot)
    prepare(0)
    for side, rows in enumerate((early, late)):
        features(rows, q_map_t, q_t.at[side], mapped_t.at[side], mapped.at[side], soft_t.at[side])
    prepare(1)
    forward_dots(0)
    for step in range(STEPS):
        if step + 2 < STEPS:
            prepare(step + 2)
        if step + 1 < STEPS:
            forward_dots(step + 1)
        forward(step)

    def settle(side, loss):
        for c in range(chunks):
            norm = 1.0 / jnp.sum(n_acc[side, c], axis=0, keepdims=True)
            student = s_acc[side, c] * norm
            mass = 1.0 / jnp.sum(l_acc[side, c], axis=0, keepdims=True)
            mismatch = student - t_acc[side, c] * mass
            upstream = 2.0 * mismatch
            gn[side, c] = (upstream * norm).astype(BF16)
            gnorm[side, c] = -jnp.sum(upstream * student, axis=0, keepdims=True) * norm
            loss = loss + jnp.sum(mismatch * mismatch, axis=0, keepdims=True)
        return loss

    loss = lax.fori_loop(0, 2, settle, jnp.zeros((1, wide), F32))
    loss_acc[...] = jnp.broadcast_to(loss[:, :BLK] + loss[:, BLK:], loss_acc.shape)

    def key_back(step):
        grad_kf = kf_bufs[step % 2]
        soft = soft_k[step]
        lead, trail = soft[:, :HD], soft[:, HD:]
        g_lead, g_trail = grad_kf[:, :HD], grad_kf[:, HD:]
        back = lead * (g_lead - jnp.sum(lead * g_lead, axis=1, keepdims=True)) - trail * (
            g_trail - jnp.sum(trail * g_trail, axis=1, keepdims=True)
        )
        high, low = split_bf16(back)
        return dot(k_t[step], high) + dot(k_t[step], low)

    def backward_dots(step):
        side, first = side_of(step), step < 2
        allowed = allowed_of(side) if first else None
        s_buf, p_buf = s_bufs.at[step % 2], p_bufs.at[step % 2]
        values = value_rows(step)
        for c in range(chunks):
            lanes = pl.ds(c * wide, wide)
            s_buf[:, lanes] = dot(values, gn[side, c])
        for c in range(chunks):
            lanes = pl.ds(c * wide, wide)
            for row in range(0, 2 * BLK, tile):
                part = s_buf[pl.ds(row, tile), lanes] + gnorm[side, c]
                if first:
                    part = jnp.where(allowed[row : row + tile], part, 0.0)
                p_buf[pl.ds(row, tile), lanes] = part.astype(BF16)

    def backward(step):
        side, first = side_of(step), step < 2
        p_buf = p_bufs.at[step % 2]
        for c in range(chunks):
            lanes = pl.ds(c * wide, wide)
            product = dot(mk_t[step], p_buf[:, lanes])
            gqf[side, c] = product if first else gqf[side, c] + product
        kf_bufs[step % 2] = dot(p_buf[...], mapped[side])

    backward_dots(0)
    gk_acc[...] = jnp.zeros((HD, HD), F32)
    for step in range(STEPS):
        if step + 1 < STEPS:
            backward_dots(step + 1)
        backward(step)
        if step:
            gk_acc[...] = gk_acc[...] + key_back(step - 1)
    flat[pl.ds(HEADS * HD, HD)] = gk_acc[...] + key_back(STEPS - 1)

    for head in range(HEADS):
        total = jnp.zeros((HD, HD), F32)
        lanes = pl.ds(head * BLK, BLK)
        column = (head % 2) * BLK
        for side in range(2):
            lead, trail = soft_t[side, :HD, lanes], soft_t[side, HD:, lanes]
            g_lead = gqf[side, head // 2, :HD, pl.ds(column, BLK)]
            g_trail = gqf[side, head // 2, HD:, pl.ds(column, BLK)]
            back = lead * (g_lead - jnp.sum(lead * g_lead, axis=0, keepdims=True)) - trail * (
                g_trail - jnp.sum(trail * g_trail, axis=0, keepdims=True)
            )
            high, low = split_bf16(back)
            rows_t = q_t[side, :, lanes]
            total = total + dot_nt(rows_t, high) + dot_nt(rows_t, low)
        flat[pl.ds(head * HD, HD)] = total
    loss_row = loss_acc[:1]
    high, low = split_bf16(loss_row)
    rest = jnp.zeros((6, BLK), F32)
    near_tail = jnp.concatenate([loss_row, jnp.zeros((1, BLK), F32), rest], axis=0)
    far_tail = jnp.concatenate([high, low, rest.astype(BF16)], axis=0)
    for chip in range(CHIPS):
        near_row = pl.multiple_of((parity * CHIPS + chip) * ROWS, 8)
        far_row = pl.multiple_of(((1 - parity) * CHIPS + chip) * ROWS, 8)
        near_out[chip, pl.ds(0, ROWS)] = flat[pl.ds(near_row, ROWS)]
        near_out[chip, pl.ds(ROWS, PAYLOAD - ROWS)] = near_tail
        far_out[chip, pl.ds(0, ROWS)] = flat[pl.ds(far_row, ROWS)].astype(BF16)
        far_out[chip, pl.ds(ROWS, PAYLOAD - ROWS)] = far_tail


def fold_kernel(pieces, chunk, stats):
    total = jnp.sum(pieces[...].astype(F32), axis=0)
    grads = total[:ROWS]
    chunk[...] = grads.astype(BF16)
    squares = jnp.sum(grads * grads, axis=0, keepdims=True)
    loss = (total[ROWS : ROWS + 1] + total[ROWS + 1 : ROWS + 2]) * (1.0 / SEQ)
    half = BLK // 2
    row = jnp.concatenate(
        [squares[:, :half] + squares[:, half:], loss[:, :half] + loss[:, half:]], axis=1
    )
    stats[...] = jnp.broadcast_to(row[None], stats.shape)


def scale_kernel(place, stats, layer0, layer1, layer2, layer3, q_out, k_out, loss, flat):
    total = jnp.sum(stats[...], axis=0)
    left = lax.broadcasted_iota(jnp.int32, (1, BLK), 1) < BLK // 2
    squared = jnp.sum(jnp.where(left, total, 0.0), axis=1, keepdims=True)
    loss[...] = jnp.sum(jnp.where(left, 0.0, total), axis=1, keepdims=True) / (
        SEQ * 2 * BLK * KV * HEADS * HD
    )
    inverse = 1.0 / jnp.sqrt(squared / ((HEADS + 1) * KV * HD * HD) + 1e-06)
    mine = place[0]
    core = lax.rem(mine, 2)
    row = lax.rem(mine // 2, 2)
    layer_at = mine // 4
    for back, ref in enumerate((layer0, layer1, layer2, layer3)):
        owner_layer = lax.rem(layer_at + 4 - back, 4)
        for number in range(4):
            owner_core = core if number < 2 else 1 - core
            owner_row = row if number % 2 == 0 else 1 - row
            piece = owner_core * CHIPS + owner_layer * 2 + owner_row
            rows = ref[pl.ds(number * ROWS, ROWS)].astype(F32) * inverse
            flat[pl.ds(pl.multiple_of(piece * ROWS, 8), ROWS)] = rows
    q_out[...] = flat[: HEADS * HD]
    k_out[...] = flat[HEADS * HD :]


def pack_kernel(keys, values, out, both, sems):
    takes = [
        pltpu.make_async_copy(keys, both.at[:, pl.ds(0, HD)], sems.at[0]),
        pltpu.make_async_copy(values, both.at[:, pl.ds(HD, HD)], sems.at[1]),
    ]
    for take in takes:
        take.start()
    for take in takes:
        take.wait()
    gives = [
        pltpu.make_async_copy(both, out.at[peer], sems.at[2 + peer]) for peer in range(CHIPS)
    ]
    for give in gives:
        give.start()
    for give in gives:
        give.wait()


def vmem():
    return pl.BlockSpec(memory_space=pltpu.VMEM)


def smem():
    return pl.BlockSpec(memory_space=pltpu.SMEM)


def shape(dims, kind):
    return jax.ShapeDtypeStruct(dims, kind)


def attend(info, same, other, k_map, early, late, q_map_t):
    wide = HEADS * BLK
    pair = 2 * BLK
    chunks = HEADS // 2
    return pl.pallas_call(
        main_kernel,
        out_shape=(shape((CHIPS, PAYLOAD, BLK), F32), shape((CHIPS, PAYLOAD, BLK), BF16)),
        in_specs=[smem()] + [vmem()] * 6,
        out_specs=(vmem(), vmem()),
        scratch_shapes=[
            pltpu.VMEM((2, HD, wide), BF16),
            pltpu.VMEM((2, 2 * HD, wide), BF16),
            pltpu.VMEM((2, wide, 2 * HD), BF16),
            pltpu.VMEM((2, 2 * HD, wide), F32),
            pltpu.VMEM((SLOTS, BLK, 2 * HD), BF16),
            pltpu.VMEM((STEPS, HD, pair), BF16),
            pltpu.VMEM((STEPS, HD, pair), BF16),
            pltpu.VMEM((STEPS, pair, 2 * HD), F32),
            pltpu.VMEM((STEPS, pair, 2 * HD), BF16),
            pltpu.VMEM((STEPS, 2 * HD, pair), BF16),
            pltpu.VMEM((2, chunks, HD, pair), F32),
            pltpu.VMEM((2, chunks, HD, pair), F32),
            pltpu.VMEM((2, chunks, 1, pair), F32),
            pltpu.VMEM((2, chunks, 8, pair), F32),
            pltpu.VMEM((2, chunks, 8, pair), F32),
            pltpu.VMEM((2, chunks, HD, pair), BF16),
            pltpu.VMEM((2, chunks, 1, pair), F32),
            pltpu.VMEM((2, chunks, 2 * HD, pair), F32),
            pltpu.VMEM((HD, HD), F32),
            pltpu.VMEM(((HEADS + 1) * HD, HD), F32),
            pltpu.VMEM((8, BLK), F32),
            pltpu.VMEM((2, pair, wide), F32),
            pltpu.VMEM((2, pair, wide), F32),
            pltpu.VMEM((2, pair, wide), BF16),
            pltpu.VMEM((2, pair, wide), BF16),
            pltpu.VMEM((2, pair, 2 * HD), F32),
            pltpu.VMEM((2, chunks, 1, pair), F32),
        ],
        compiler_params=pltpu.CompilerParams(vmem_limit_bytes=ATTEND_VMEM),
        name="attend",
    )(info, same, other, k_map, early, late, q_map_t)


def layer(queries, keys, values, q_map, k_map, block_pairs):
    place = lax.axis_index("seq").astype(jnp.int32).reshape(1)
    sent = pl.pallas_call(
        pack_kernel,
        out_shape=shape((CHIPS, 2 * BLK, 2 * HD), BF16),
        in_specs=[pl.BlockSpec(memory_space=pl.ANY)] * 2,
        out_specs=pl.BlockSpec(memory_space=pl.ANY),
        scratch_shapes=[
            pltpu.VMEM((2 * BLK, 2 * HD), BF16),
            pltpu.SemaphoreType.DMA((2 + CHIPS,)),
        ],
        compiler_params=pltpu.CompilerParams(vmem_limit_bytes=56 * 1024 * 1024),
        name="pack",
    )(keys[:, 0, :], values[:, 0, :])
    same = lax.all_to_all(sent, "seq", 0, 0, axis_index_groups=SAME_CORE, tiled=True)
    other = lax.ppermute(same, "seq", OTHER_CORE)

    early = jnp.transpose(queries[:BLK], (1, 0, 2))
    late = jnp.transpose(queries[BLK:], (1, 0, 2))
    late = lax.ppermute(late, "seq", MIRROR)
    q_map_t = jnp.transpose(q_map, (0, 2, 1))
    info = pl.pallas_call(
        list_kernel,
        out_shape=shape((128,), jnp.int32),
        in_specs=[smem(), smem()],
        out_specs=smem(),
        cost_estimate=pl.CostEstimate(flops=5 * 10**9, bytes_accessed=10**5, transcendentals=0),
        compiler_params=pltpu.CompilerParams(vmem_limit_bytes=SMALL_VMEM),
        name="list",
    )(place, block_pairs.reshape(-1))

    small = pltpu.CompilerParams(vmem_limit_bytes=SMALL_VMEM)
    near, far = attend(info, same, other, k_map[0], early, late, q_map_t)
    met = (near + lax.ppermute(far, "seq", OTHER_CORE).astype(F32)).astype(BF16)
    pieces = lax.all_to_all(met, "seq", 0, 0, axis_index_groups=SAME_CORE, tiled=True)
    everyone = SEQ * KV
    chunk, stats = pl.pallas_call(
        fold_kernel,
        out_shape=(shape((ROWS, BLK), BF16), shape((everyone, 1, BLK), F32)),
        in_specs=[vmem()],
        out_specs=(vmem(), vmem()),
        compiler_params=small,
        name="fold",
    )(pieces)
    stats = lax.all_to_all(stats, ("seq", "kv"), 0, 0, tiled=True)
    across = lax.ppermute(chunk, "seq", OTHER_ROW)
    aside = lax.ppermute(chunk, "seq", OTHER_CORE)
    diagonal = lax.ppermute(across, "seq", OTHER_CORE)
    near = jnp.concatenate([chunk, across, aside, diagonal], axis=0)
    layers = [near] + [lax.ppermute(near, "seq", route) for route in LAYER_SHIFTS]
    grad_q, grad_k, loss = pl.pallas_call(
        scale_kernel,
        out_shape=(shape((HEADS * HD, HD), F32), shape((HD, HD), F32), shape((1, 1), F32)),
        in_specs=[smem()] + [vmem()] * 5,
        out_specs=(vmem(), vmem(), vmem()),
        scratch_shapes=[pltpu.VMEM(((HEADS + 1) * HD, HD), F32)],
        compiler_params=small,
        name="scale",
    )(place, stats, *layers)
    return grad_q.reshape(HEADS, HD, HD), grad_k.reshape(1, HD, HD), loss.reshape(())


def solution(mesh):
    placed = (
        P("seq", "kv", None),
        P("seq", "kv", None),
        P("seq", "kv", None),
        P("kv", None, None),
        P("kv", None, None),
        P(),
    )
    return jax.shard_map(
        layer,
        mesh=mesh,
        in_specs=placed,
        out_specs=(P("kv", None, None), P("kv", None, None), P()),
        check_vma=False,
    )
```

```python
import math

import jax
import jax.numpy as jnp
from jax import lax
from jax.experimental import pallas as pl
from jax.experimental.pallas import tpu as pltpu
from jax.sharding import PartitionSpec as P


BLK = 128
HD = 128
HEADS = 8
SEQ = 16
KV = 8
CHIPS = SEQ // 2
SLOTS = 18
STEPS = SLOTS // 2
ATTEND_VMEM = 34 * 1024 * 1024
SMALL_VMEM = 4 * 1024 * 1024
FLOOR = -1e30
LOG2E = 1.4426950408889634
ROWS = 72
PAYLOAD = 80
BF16 = jnp.bfloat16
F32 = jnp.float32

SAME_CORE = [[core + 2 * chip for chip in range(SEQ // 2)] for core in range(2)]
OTHER_CORE = [(i, i ^ 1) for i in range(SEQ)]
OTHER_ROW = [(i, i ^ 2) for i in range(SEQ)]
LAYER_SHIFTS = [[(i, (i + 4 * back) % SEQ) for i in range(SEQ)] for back in (1, 2, 3)]
MIRROR = [(i, SEQ - 1 - i) for i in range(SEQ)]


def dot(a, b):
    return jnp.dot(a, b, preferred_element_type=F32)


def dot_nt(a, b):
    return lax.dot_general(a, b, (((1,), (1,)), ((), ())), preferred_element_type=F32)


def split_bf16(x):
    high = x.astype(BF16)
    return high, (x - high.astype(F32)).astype(BF16)


def halves(u, axis):
    top = jnp.max(u, axis=axis, keepdims=True)
    low = jnp.min(u, axis=axis, keepdims=True)
    up = jnp.exp(u - top)
    down = jnp.exp(low - u)
    up = up / jnp.sum(up, axis=axis, keepdims=True)
    down = down / jnp.sum(down, axis=axis, keepdims=True)
    return up, down


def list_blocks(mine, pairs, info):
    late = 2 * (SEQ - 1 - mine) + 1
    odd = lax.rem(mine, 2)
    for slot in range(SLOTS):
        info[slot] = 0
    info[0] = 2 * mine
    info[2] = late
    late_first = 4 + 2 * (mine // 2)

    def scan(row, counts):
        early_count, late_count = counts
        query = pairs[2 * row]
        key = pairs[2 * row + 1]
        earlier = query != key
        is_early = (query == 2 * mine) & earlier
        is_late = (query == late) & earlier

        @pl.when(is_early | is_late)
        def _():
            early_slot = jnp.where(early_count < odd, 1, 4 + early_count - odd)
            late_slot = jnp.where(late_count < 1 - odd, 3, late_first + late_count - (1 - odd))
            info[jnp.minimum(jnp.where(is_early, early_slot, late_slot), SLOTS - 1)] = key

        return (
            early_count + jnp.where(is_early, 1, 0),
            late_count + jnp.where(is_late, 1, 0),
        )

    lax.fori_loop(0, pairs.shape[0] // 2, scan, (jnp.int32(0), jnp.int32(0)))
    info[32] = jnp.where(odd == 1, 2 * BLK, -2 * BLK)
    info[33] = jnp.where(odd == 1, -2 * BLK, 2 * BLK)
    info[34] = 2 + mine // 2
    info[35] = odd


def features(q, q_map_t, q_t, mapped_t, mapped, soft_t):
    for head in range(HEADS):
        lanes = pl.ds(head * BLK, BLK)
        rows_t = q[head].T
        q_t[:, lanes] = rows_t
        up, down = halves(dot(q_map_t[head], rows_t), 0)
        soft = jnp.concatenate([up, down], axis=0)
        soft_t[:, lanes] = soft
        rounded = soft.astype(BF16)
        mapped_t[:, lanes] = rounded
        mapped[lanes, :] = rounded.T


def list_kernel(place, pairs, info):
    list_blocks(place[0], pairs, info)


def main_kernel(
    info, same, other, k_map, early, late, q_map_t,
    near_out, far_out,
    q_t, mapped_t, mapped, soft_t, kv, v_t, k_t, soft_k, mk, mk_t,
    t_acc, s_acc, m_acc, l_acc, n_acc, gn, gnorm, gqf, gk_acc, flat, loss_acc,
    s_bufs, x_raws, p_bufs, x_bufs, kf_bufs, shift_bufs,
):
    parity = info[35]
    switch = info[34]

    def fetch(slot):
        block = info[slot]
        chip = block // 4
        rows = pl.ds(pl.multiple_of(lax.rem(block, 2) * BLK, BLK), BLK)
        near = lax.rem(block // 2, 2) == parity
        kv[slot] = jnp.where(near, same[chip, rows], other[chip, rows])

    def key_rows(step):
        return jnp.concatenate([kv[2 * step, :, :HD], kv[2 * step + 1, :, :HD]], axis=0)

    def value_rows(step):
        return jnp.concatenate([kv[2 * step, :, HD:], kv[2 * step + 1, :, HD:]], axis=0)

    def prepare(step):
        keys = key_rows(step)
        up, down = halves(dot(keys, k_map[...]), 1)
        soft_k[step, :, :HD] = up
        soft_k[step, :, HD:] = down
        up = up.astype(BF16)
        down = down.astype(BF16)
        mk[step, :, :HD] = up
        mk[step, :, HD:] = down
        mk_t[step, :HD] = up.T
        mk_t[step, HD:] = down.T
        v_t[step, :HD] = value_rows(step).T
        v_t[step, HD:] = jnp.ones((16, 2 * BLK), BF16)
        k_t[step] = keys.T

    def allowed_of(side):
        key_minus_query = lax.broadcasted_iota(jnp.int32, (BLK, BLK), 0) - (
            lax.broadcasted_iota(jnp.int32, (BLK, BLK), 1)
        )
        tall = jnp.concatenate(
            [key_minus_query <= 0, key_minus_query <= info[32 + side]], axis=0
        )
        return jnp.concatenate([tall, tall], axis=1)

    shrink = LOG2E / math.sqrt(HD)
    wide = 2 * BLK
    chunks = HEADS // 2

    tile = 64

    def over_sublanes(x, fold):
        return fold(x.reshape(x.shape[0] // 8, 8, x.shape[1]), axis=0)

    def side_of(step):
        if step < 2:
            return step
        return jnp.where(step >= switch, 1, 0)

    def forward_dots(step):
        side = side_of(step)
        s_buf, x_raw = s_bufs.at[step % 2], x_raws.at[step % 2]
        keys = key_rows(step)
        for c in range(chunks):
            lanes = pl.ds(c * wide, wide)
            s_buf[:, lanes] = dot(keys, q_t[side, :, lanes])
        for c in range(chunks):
            lanes = pl.ds(c * wide, wide)
            x_raw[:, lanes] = dot(mk[step], mapped_t[side, :, lanes])

    def forward(step):
        side, first = side_of(step), step < 2
        allowed = allowed_of(side) if first else None
        s_buf, x_raw = s_bufs.at[step % 2], x_raws.at[step % 2]
        p_buf, x_buf = p_bufs.at[step % 2], x_bufs.at[step % 2]
        shift_buf = shift_bufs.at[step % 2]

        def masked(part, row, other):
            return jnp.where(allowed[row : row + tile], part, other) if first else part

        for c in range(chunks):
            lanes = pl.ds(c * wide, wide)
            best = jnp.full((8, wide), FLOOR, F32)
            for row in range(0, 2 * BLK, tile):
                part = masked(s_buf[pl.ds(row, tile), lanes], row, FLOOR)
                best = jnp.maximum(best, over_sublanes(part, jnp.max))
            new = jnp.max(best, axis=0, keepdims=True)
            if first:
                m_acc[side, c] = new
            else:
                old = m_acc[side, c]
                new = jnp.maximum(old, new)
                m_acc[side, c] = new
                shift = jnp.exp2((old - new) * shrink)
                shift_buf[c] = shift
            for row in range(0, 2 * BLK, tile):
                part = masked(s_buf[pl.ds(row, tile), lanes], row, FLOOR)
                weights = jnp.exp2((part - new) * shrink)
                p_buf[pl.ds(row, tile), lanes] = weights.astype(BF16)
        for c in range(chunks):
            lanes = pl.ds(c * wide, wide)
            for row in range(0, 2 * BLK, tile):
                part = masked(x_raw[pl.ds(row, tile), lanes], row, 0.0)
                x_buf[pl.ds(row, tile), lanes] = part.astype(BF16)
        for c in range(chunks):
            lanes = pl.ds(c * wide, wide)
            product = dot(v_t[step], x_buf[:, lanes])
            total, product = product[HD : HD + 8], product[:HD]
            n_acc[side, c] = total if first else n_acc[side, c] + total
            s_acc[side, c] = product if first else s_acc[side, c] + product
        for c in range(chunks):
            lanes = pl.ds(c * wide, wide)
            product = dot(v_t[step], p_buf[:, lanes])
            total, product = product[HD : HD + 8], product[:HD]
            l_acc[side, c] = total if first else l_acc[side, c] * shift_buf[c] + total
            t_acc[side, c] = product if first else t_acc[side, c] * shift_buf[c] + product

    for slot in range(SLOTS):
        fetch(slot)
    prepare(0)
    for side, rows in enumerate((early, late)):
        features(rows, q_map_t, q_t.at[side], mapped_t.at[side], mapped.at[side], soft_t.at[side])
    prepare(1)
    forward_dots(0)
    for step in range(STEPS):
        if step + 2 < STEPS:
            prepare(step + 2)
        if step + 1 < STEPS:
            forward_dots(step + 1)
        forward(step)

    def settle(side, loss):
        for c in range(chunks):
            norm = 1.0 / n_acc[side, c][:1]
            student = s_acc[side, c] * norm
            mass = 1.0 / l_acc[side, c][:1]
            mismatch = student - t_acc[side, c] * mass
            upstream = 2.0 * mismatch
            gn[side, c] = (upstream * norm).astype(BF16)
            gnorm[side, c] = -jnp.sum(upstream * student, axis=0, keepdims=True) * norm
            loss = loss + jnp.sum(mismatch * mismatch, axis=0, keepdims=True)
        return loss

    loss = lax.fori_loop(0, 2, settle, jnp.zeros((1, wide), F32))
    loss_acc[...] = jnp.broadcast_to(loss[:, :BLK] + loss[:, BLK:], loss_acc.shape)

    def key_back(step):
        grad_kf = kf_bufs[step % 2]
        soft = soft_k[step]
        lead, trail = soft[:, :HD], soft[:, HD:]
        g_lead, g_trail = grad_kf[:, :HD], grad_kf[:, HD:]
        back = lead * (g_lead - jnp.sum(lead * g_lead, axis=1, keepdims=True)) - trail * (
            g_trail - jnp.sum(trail * g_trail, axis=1, keepdims=True)
        )
        high, low = split_bf16(back)
        return dot(k_t[step], high) + dot(k_t[step], low)

    def backward_dots(step):
        side, first = side_of(step), step < 2
        allowed = allowed_of(side) if first else None
        s_buf, p_buf = s_bufs.at[step % 2], p_bufs.at[step % 2]
        values = value_rows(step)
        for c in range(chunks):
            lanes = pl.ds(c * wide, wide)
            s_buf[:, lanes] = dot(values, gn[side, c])
        for c in range(chunks):
            lanes = pl.ds(c * wide, wide)
            for row in range(0, 2 * BLK, tile):
                part = s_buf[pl.ds(row, tile), lanes] + gnorm[side, c]
                if first:
                    part = jnp.where(allowed[row : row + tile], part, 0.0)
                p_buf[pl.ds(row, tile), lanes] = part.astype(BF16)

    def backward(step):
        side, first = side_of(step), step < 2
        p_buf = p_bufs.at[step % 2]
        for c in range(chunks):
            lanes = pl.ds(c * wide, wide)
            product = dot(mk_t[step], p_buf[:, lanes])
            gqf[side, c] = product if first else gqf[side, c] + product
        kf_bufs[step % 2] = dot(p_buf[...], mapped[side])

    backward_dots(0)
    gk_acc[...] = jnp.zeros((HD, HD), F32)
    for step in range(STEPS):
        if step + 1 < STEPS:
            backward_dots(step + 1)
        backward(step)
        if step:
            gk_acc[...] = gk_acc[...] + key_back(step - 1)
    flat[pl.ds(HEADS * HD, HD)] = gk_acc[...] + key_back(STEPS - 1)

    for head in range(HEADS):
        total = jnp.zeros((HD, HD), F32)
        lanes = pl.ds(head * BLK, BLK)
        column = (head % 2) * BLK
        for side in range(2):
            lead, trail = soft_t[side, :HD, lanes], soft_t[side, HD:, lanes]
            g_lead = gqf[side, head // 2, :HD, pl.ds(column, BLK)]
            g_trail = gqf[side, head // 2, HD:, pl.ds(column, BLK)]
            back = lead * (g_lead - jnp.sum(lead * g_lead, axis=0, keepdims=True)) - trail * (
                g_trail - jnp.sum(trail * g_trail, axis=0, keepdims=True)
            )
            high, low = split_bf16(back)
            rows_t = q_t[side, :, lanes]
            total = total + dot_nt(rows_t, high) + dot_nt(rows_t, low)
        flat[pl.ds(head * HD, HD)] = total
    loss_row = loss_acc[:1]
    high, low = split_bf16(loss_row)
    rest = jnp.zeros((6, BLK), F32)
    near_tail = jnp.concatenate([loss_row, jnp.zeros((1, BLK), F32), rest], axis=0)
    far_tail = jnp.concatenate([high, low, rest.astype(BF16)], axis=0)
    for chip in range(CHIPS):
        near_row = pl.multiple_of((parity * CHIPS + chip) * ROWS, 8)
        far_row = pl.multiple_of(((1 - parity) * CHIPS + chip) * ROWS, 8)
        near_out[chip, pl.ds(0, ROWS)] = flat[pl.ds(near_row, ROWS)]
        near_out[chip, pl.ds(ROWS, PAYLOAD - ROWS)] = near_tail
        far_out[chip, pl.ds(0, ROWS)] = flat[pl.ds(far_row, ROWS)].astype(BF16)
        far_out[chip, pl.ds(ROWS, PAYLOAD - ROWS)] = far_tail


def fold_kernel(pieces, chunk, stats):
    total = jnp.sum(pieces[...].astype(F32), axis=0)
    grads = total[:ROWS]
    chunk[...] = grads.astype(BF16)
    squares = jnp.sum(grads * grads, axis=0, keepdims=True)
    loss = (total[ROWS : ROWS + 1] + total[ROWS + 1 : ROWS + 2]) * (1.0 / SEQ)
    half = BLK // 2
    row = jnp.concatenate(
        [squares[:, :half] + squares[:, half:], loss[:, :half] + loss[:, half:]], axis=1
    )
    stats[...] = jnp.broadcast_to(row[None], stats.shape)


def scale_kernel(place, stats, layer0, layer1, layer2, layer3, q_out, k_out, loss, flat):
    total = jnp.sum(stats[...], axis=0)
    left = lax.broadcasted_iota(jnp.int32, (1, BLK), 1) < BLK // 2
    squared = jnp.sum(jnp.where(left, total, 0.0), axis=1, keepdims=True)
    loss[...] = jnp.sum(jnp.where(left, 0.0, total), axis=1, keepdims=True) / (
        SEQ * 2 * BLK * KV * HEADS * HD
    )
    inverse = 1.0 / jnp.sqrt(squared / ((HEADS + 1) * KV * HD * HD) + 1e-06)
    mine = place[0]
    core = lax.rem(mine, 2)
    row = lax.rem(mine // 2, 2)
    layer_at = mine // 4
    for back, ref in enumerate((layer0, layer1, layer2, layer3)):
        owner_layer = lax.rem(layer_at + 4 - back, 4)
        for number in range(4):
            owner_core = core if number < 2 else 1 - core
            owner_row = row if number % 2 == 0 else 1 - row
            piece = owner_core * CHIPS + owner_layer * 2 + owner_row
            rows = ref[pl.ds(number * ROWS, ROWS)].astype(F32) * inverse
            flat[pl.ds(pl.multiple_of(piece * ROWS, 8), ROWS)] = rows
    q_out[...] = flat[: HEADS * HD]
    k_out[...] = flat[HEADS * HD :]


def pack_kernel(keys, values, out, both, sems):
    takes = [
        pltpu.make_async_copy(keys, both.at[:, pl.ds(0, HD)], sems.at[0]),
        pltpu.make_async_copy(values, both.at[:, pl.ds(HD, HD)], sems.at[1]),
    ]
    for take in takes:
        take.start()
    for take in takes:
        take.wait()
    gives = [
        pltpu.make_async_copy(both, out.at[peer], sems.at[2 + peer]) for peer in range(CHIPS)
    ]
    for give in gives:
        give.start()
    for give in gives:
        give.wait()


def vmem():
    return pl.BlockSpec(memory_space=pltpu.VMEM)


def smem():
    return pl.BlockSpec(memory_space=pltpu.SMEM)


def shape(dims, kind):
    return jax.ShapeDtypeStruct(dims, kind)


def attend(info, same, other, k_map, early, late, q_map_t):
    wide = HEADS * BLK
    pair = 2 * BLK
    chunks = HEADS // 2
    return pl.pallas_call(
        main_kernel,
        out_shape=(shape((CHIPS, PAYLOAD, BLK), F32), shape((CHIPS, PAYLOAD, BLK), BF16)),
        in_specs=[smem()] + [vmem()] * 6,
        out_specs=(vmem(), vmem()),
        scratch_shapes=[
            pltpu.VMEM((2, HD, wide), BF16),
            pltpu.VMEM((2, 2 * HD, wide), BF16),
            pltpu.VMEM((2, wide, 2 * HD), BF16),
            pltpu.VMEM((2, 2 * HD, wide), F32),
            pltpu.VMEM((SLOTS, BLK, 2 * HD), BF16),
            pltpu.VMEM((STEPS, HD + 16, pair), BF16),
            pltpu.VMEM((STEPS, HD, pair), BF16),
            pltpu.VMEM((STEPS, pair, 2 * HD), F32),
            pltpu.VMEM((STEPS, pair, 2 * HD), BF16),
            pltpu.VMEM((STEPS, 2 * HD, pair), BF16),
            pltpu.VMEM((2, chunks, HD, pair), F32),
            pltpu.VMEM((2, chunks, HD, pair), F32),
            pltpu.VMEM((2, chunks, 1, pair), F32),
            pltpu.VMEM((2, chunks, 8, pair), F32),
            pltpu.VMEM((2, chunks, 8, pair), F32),
            pltpu.VMEM((2, chunks, HD, pair), BF16),
            pltpu.VMEM((2, chunks, 1, pair), F32),
            pltpu.VMEM((2, chunks, 2 * HD, pair), F32),
            pltpu.VMEM((HD, HD), F32),
            pltpu.VMEM(((HEADS + 1) * HD, HD), F32),
            pltpu.VMEM((8, BLK), F32),
            pltpu.VMEM((2, pair, wide), F32),
            pltpu.VMEM((2, pair, wide), F32),
            pltpu.VMEM((2, pair, wide), BF16),
            pltpu.VMEM((2, pair, wide), BF16),
            pltpu.VMEM((2, pair, 2 * HD), F32),
            pltpu.VMEM((2, chunks, 1, pair), F32),
        ],
        compiler_params=pltpu.CompilerParams(vmem_limit_bytes=ATTEND_VMEM),
        name="attend",
    )(info, same, other, k_map, early, late, q_map_t)


def layer(queries, keys, values, q_map, k_map, block_pairs):
    place = lax.axis_index("seq").astype(jnp.int32).reshape(1)
    sent = pl.pallas_call(
        pack_kernel,
        out_shape=shape((CHIPS, 2 * BLK, 2 * HD), BF16),
        in_specs=[pl.BlockSpec(memory_space=pl.ANY)] * 2,
        out_specs=pl.BlockSpec(memory_space=pl.ANY),
        scratch_shapes=[
            pltpu.VMEM((2 * BLK, 2 * HD), BF16),
            pltpu.SemaphoreType.DMA((2 + CHIPS,)),
        ],
        compiler_params=pltpu.CompilerParams(vmem_limit_bytes=56 * 1024 * 1024),
        name="pack",
    )(keys[:, 0, :], values[:, 0, :])
    same = lax.all_to_all(sent, "seq", 0, 0, axis_index_groups=SAME_CORE, tiled=True)
    other = lax.ppermute(same, "seq", OTHER_CORE)

    early = jnp.transpose(queries[:BLK], (1, 0, 2))
    late = jnp.transpose(queries[BLK:], (1, 0, 2))
    late = lax.ppermute(late, "seq", MIRROR)
    q_map_t = jnp.transpose(q_map, (0, 2, 1))
    info = pl.pallas_call(
        list_kernel,
        out_shape=shape((128,), jnp.int32),
        in_specs=[smem(), smem()],
        out_specs=smem(),
        cost_estimate=pl.CostEstimate(flops=5 * 10**9, bytes_accessed=10**5, transcendentals=0),
        compiler_params=pltpu.CompilerParams(vmem_limit_bytes=SMALL_VMEM),
        name="list",
    )(place, block_pairs.reshape(-1))

    small = pltpu.CompilerParams(vmem_limit_bytes=SMALL_VMEM)
    near, far = attend(info, same, other, k_map[0], early, late, q_map_t)
    met = (near + lax.ppermute(far, "seq", OTHER_CORE).astype(F32)).astype(BF16)
    pieces = lax.all_to_all(met, "seq", 0, 0, axis_index_groups=SAME_CORE, tiled=True)
    everyone = SEQ * KV
    chunk, stats = pl.pallas_call(
        fold_kernel,
        out_shape=(shape((ROWS, BLK), BF16), shape((everyone, 1, BLK), F32)),
        in_specs=[vmem()],
        out_specs=(vmem(), vmem()),
        compiler_params=small,
        name="fold",
    )(pieces)
    stats = lax.all_to_all(stats, ("seq", "kv"), 0, 0, tiled=True)
    across = lax.ppermute(chunk, "seq", OTHER_ROW)
    aside = lax.ppermute(chunk, "seq", OTHER_CORE)
    diagonal = lax.ppermute(across, "seq", OTHER_CORE)
    near = jnp.concatenate([chunk, across, aside, diagonal], axis=0)
    layers = [near] + [lax.ppermute(near, "seq", route) for route in LAYER_SHIFTS]
    grad_q, grad_k, loss = pl.pallas_call(
        scale_kernel,
        out_shape=(shape((HEADS * HD, HD), F32), shape((HD, HD), F32), shape((1, 1), F32)),
        in_specs=[smem()] + [vmem()] * 5,
        out_specs=(vmem(), vmem(), vmem()),
        scratch_shapes=[pltpu.VMEM(((HEADS + 1) * HD, HD), F32)],
        compiler_params=small,
        name="scale",
    )(place, stats, *layers)
    return grad_q.reshape(HEADS, HD, HD), grad_k.reshape(1, HD, HD), loss.reshape(())


def solution(mesh):
    placed = (
        P("seq", "kv", None),
        P("seq", "kv", None),
        P("seq", "kv", None),
        P("kv", None, None),
        P("kv", None, None),
        P(),
    )
    return jax.shard_map(
        layer,
        mesh=mesh,
        in_specs=placed,
        out_specs=(P("kv", None, None), P("kv", None, None), P()),
        check_vma=False,
    )
```
